128 devices in a mesh: blk: 4 (over y), mp: 16 (over x, z), kv: 2 (over core).
Axes of the slice: x: 4, y: 4, z: 4, core: 2. Of those that a mesh axis runs over, the one named last changes fastest.
Arguments:
- tokens: bfloat16 [2048, 16384], P(('blk', 'kv'), 'mp'), may hold values from -21 to 21, as said below
- norm_gain: bfloat16 [16384], P('mp'), may hold values from 0.099609375 to 1.8984375
- query_weight: bfloat16 [16384, 16384], P('mp', 'blk'), may hold values from -0.53125 to 0.53125, as said below
- key_weight: bfloat16 [16384, 1024], P('mp', 'blk'), may hold values from -0.03125 to 0.03125, as said below
- documents: int32 [2048], replicated, may hold values from 0 to 3, never falling along the last dimension, each value on 1 to 1024 neighbouring positions
- span_ids: int32 [2048], replicated, may hold values from 0 to 1023, never falling along the last dimension, each value on 1 to 4 neighbouring positions
Outputs:
- span_logmap: float32 [1024, 128, 1024], P('kv', ('blk', 'mp'))
The draws below stay inside these ranges and needn't reach their ends.
Inputs may be any that keep to these rules, and one draw needn't show every extreme that they name: `tokens`: custom draw; values are real-valued activations. `query_weight`: custom draw of fan-in scale. `key_weight`: custom draw of fan-in scale. `documents`: never falling along the tokens; each of the 4 documents covers 1 to 1024 consecutive tokens, one exactly 1024. `span_ids`: never falling along the tokens; each of the 1024 spans covers 1 to 4 consecutive tokens, one exactly 4.
All inputs are finite; a program needn't handle non-finite values.
Results may differ from the reference program's by a relative error of at most 0.0006.
Values may be sent and summed in bfloat16 or wider, within the bound.
A program may use at most 128 MiB of HBM per device.

```python
import math
import jax
import jax.numpy as jnp
import numpy as np
from jax import lax

D = 16384
HQ = 128
KVH = 8
HD = 128
DOCS = 4
SPAN_MOST = 4
TOKENS = 2048
NS = 1024
DOC_MOST = 1024


def draw_tokens(key, part):
    key = jax.random.fold_in(key, 11)
    first_key = jax.random.fold_in(key, 0)
    column = jnp.arange(D, dtype=jnp.float32)
    col_scale = 0.4 * jnp.power(10.0, column / D)
    activations = jnp.clip(jax.random.normal(first_key, (TOKENS, D), jnp.float32), -5.0, 5.0) * col_scale[None, :]
    return activations.astype(jnp.bfloat16)


def key_matrix(key):
    inner_key = jax.random.fold_in(key, 29)
    sample = jnp.clip(jax.random.normal(inner_key, (D, KVH * HD), jnp.float32), -4.0, 4.0)
    return sample / jnp.sqrt(jnp.float32(D))


def draw_key_weight(key, part):
    return key_matrix(key).astype(jnp.bfloat16)


def draw_query_weight(key, part):
    first_key = jax.random.fold_in(jax.random.fold_in(key, 31), 0)
    sample = jnp.clip(jax.random.normal(first_key, (D, HQ * HD), jnp.float32), -4.0, 4.0) / jnp.sqrt(jnp.float32(D))
    return sample.astype(jnp.bfloat16)


def length_profile(amount, total, most, slope):
    portions = [(1 << 20) // math.isqrt(rank ** slope) + 1 for rank in range(2, amount + 1)]
    rest, holding = total - most - (amount - 1), [1] * (amount - 1)
    while rest > 0:
        candidates = [i for i in range(amount - 1) if holding[i] < most]
        pool, left = sum([portions[i] for i in candidates]), rest
        for i in candidates:
            more = min(most - holding[i], max(1, left * portions[i] // pool), rest)
            holding[i] = holding[i] + more
            rest = rest - more
    return np.array([most] + holding)


def ragged_sizes(rng, number_of, total, most, slope):
    if number_of == 2:
        one = jax.random.randint(rng, (), max(1, total - most), min(most, total - 1) + 1)
        return jnp.stack([one, total - one])
    tallies = jnp.asarray(length_profile(number_of, total, most, slope), jnp.int32)
    couples = (number_of - 1) // 2
    source_of, sink = tallies[1:1 + 2 * couples:2], tallies[2:2 + 2 * couples:2]
    slack = jnp.minimum(source_of - 1, most - sink)
    passed = jax.random.randint(jax.random.fold_in(rng, 1), (couples,), 0, 1 << 20) % (slack + 1)
    tallies = tallies.at[1:1 + 2 * couples:2].set(source_of - passed).at[2:2 + 2 * couples:2].set(sink + passed)
    return tallies[jax.random.permutation(jax.random.fold_in(rng, 2), number_of)]


def setup_inputs(seed: int = 0) -> dict:
    splits = jax.random.split(jax.random.key(seed), 7)
    return {
        "tokens": draw_tokens(jax.random.fold_in(splits[6], 71), 0),
        "norm_gain": jnp.clip(1.0 + 0.18 * jax.random.normal(splits[1], (D,), jnp.float32), 0.099609375, 1.8984375).astype(jnp.bfloat16),
        "query_weight": draw_query_weight(jax.random.fold_in(splits[6], 71), 0),
        "key_weight": draw_key_weight(jax.random.fold_in(splits[6], 71), 0),
        "documents": jnp.searchsorted(jnp.cumsum(ragged_sizes(splits[4], DOCS, TOKENS, DOC_MOST, 2)), jnp.arange(TOKENS), side="right").astype(jnp.int32),
        "span_ids": jnp.searchsorted(jnp.cumsum(ragged_sizes(splits[5], NS, TOKENS, SPAN_MOST, 2)), jnp.arange(TOKENS), side="right").astype(jnp.int32),
    }


def rope_freqs(half_width):
    iota_index = jnp.arange(half_width, dtype=jnp.float32)
    base_freq = jnp.power(500000.0, -iota_index / half_width)
    wavelen = 2.0 * jnp.pi / base_freq
    smooth = (8192.0 / wavelen - 1.0) / 3.0
    blended = (1.0 - smooth) * base_freq / 8.0 + smooth * base_freq
    return jnp.where(wavelen < 2048.0, base_freq, jnp.where(wavelen > 8192.0, base_freq / 8.0, blended))

def rotate(vectors, cosine, sine_table):
    half_width = vectors.shape[-1] // 2
    first_half = vectors[..., :half_width]
    second_half = vectors[..., half_width:]
    return jnp.concatenate([first_half * cosine - second_half * sine_table, second_half * cosine + first_half * sine_table], axis=-1)

def doc_positions(documents):
    onehot = (documents[:, None] == jnp.arange(DOCS, dtype=jnp.int32)[None, :]).astype(jnp.int32)
    counts = lax.optimization_barrier(jnp.sum(onehot, axis=0))
    starts = jnp.cumsum(counts) - counts
    return jnp.arange(documents.shape[0], dtype=jnp.int32) - lax.optimization_barrier(jnp.sum(onehot * starts[None, :], axis=1))

def angles(positions):
    frequency = rope_freqs(HD // 2)
    phase_angle = positions.astype(jnp.float32)[:, None] * frequency[None, :]
    return (jnp.cos(phase_angle), jnp.sin(phase_angle))

def reference(tokens, norm_gain, query_weight, key_weight, documents, span_ids):
    activations = tokens.astype(jnp.float32)
    row_squares = lax.optimization_barrier(jnp.sum(activations * activations, axis=1))
    normed = (activations * lax.rsqrt(row_squares / D + 1e-05)[:, None] * norm_gain.astype(jnp.float32)[None, :]).astype(jnp.bfloat16)
    query_raw = jnp.dot(normed, query_weight, preferred_element_type=jnp.float32).reshape(TOKENS, HQ, HD)
    key_raw = jnp.dot(normed, key_weight, preferred_element_type=jnp.float32).reshape(TOKENS, KVH, HD)
    cosine, sine_table = angles(doc_positions(documents))
    queries = rotate(query_raw, cosine[:, None, :], sine_table[:, None, :]).astype(jnp.bfloat16)
    keys_rotated = rotate(key_raw, cosine[:, None, :], sine_table[:, None, :]).astype(jnp.bfloat16)
    token_order = jnp.arange(TOKENS, dtype=jnp.int32)
    visible = (documents[:, None] == documents[None, :]) & (token_order[None, :] <= token_order[:, None])
    span_match = span_ids[:, None] == jnp.arange(NS, dtype=jnp.int32)[None, :]
    onehot = span_match.astype(jnp.bfloat16)
    span_counts = lax.optimization_barrier(jnp.sum(span_match.astype(jnp.float32), axis=0))
    scale_factor = 1.0 / math.sqrt(HD)

    def one_head(head_index):
        query_head = lax.dynamic_index_in_dim(queries, head_index, 1, keepdims=False)
        key_head = lax.dynamic_index_in_dim(keys_rotated, head_index // (HQ // KVH), 1, keepdims=False)
        scores = jnp.dot(query_head, key_head.T, preferred_element_type=jnp.float32) * scale_factor
        peak_score = lax.optimization_barrier(jnp.max(jnp.where(visible, scores, -jnp.inf), axis=1, keepdims=True))
        weights = jnp.exp(jnp.where(visible, scores - peak_score, -jnp.inf))
        attn_probs = (weights / lax.optimization_barrier(jnp.sum(weights, axis=1, keepdims=True))).astype(jnp.bfloat16)
        key_mass = jnp.dot(attn_probs, onehot, preferred_element_type=jnp.float32).astype(jnp.bfloat16)
        return jnp.dot(onehot.T, key_mass, preferred_element_type=jnp.float32)
    totals = lax.map(one_head, jnp.arange(HQ, dtype=jnp.int32))
    span_total = jnp.transpose(totals, (1, 0, 2))
    return jnp.log(span_total / span_counts[:, None, None] + 1e-06)
```

```python
import functools
import math

import jax
import jax.numpy as jnp
import numpy as np
from jax import lax
from jax.experimental import pallas as pl
from jax.experimental.pallas import tpu as pltpu
from jax.sharding import Mesh
from jax.sharding import PartitionSpec as P

D = 16384
HD = 128
TOKENS = 2048
NS = 1024
X, Z, Y, CORE = "mp_0", "mp_1", "blk", "kv"
MP = (X, Z)
BLK_MP = (Y, X, Z)
MESH = pl.DeviceIdType.MESH
F32 = jnp.float32
BF16 = jnp.bfloat16
RING = 4
CH = 8
R = 128
KI = 4
LAST = CH + 4
SLOT_A = {2: 0, 1: 2, 3: 1, 0: 3}
SLOT_B = {2: 1, 1: 0, 3: 2, 0: 3}
ORDER = (2, 1, 3, 0)
PEERS = [(ox, oz) for ox in range(4) for oz in range(4) if (ox, oz) != (0, 0)]


def step(pos, by):
    return lax.rem(pos + by, RING)


def piece_of(i):
    half = lax.rem(i + i // 4 + i // 6, 2)
    far = i // 6
    other = (i + 4) // 6
    offset = other * (1 - far) * (3 - 2 * lax.rem(i, 2)) + 2 * far
    return offset, half


def first_send(st, r, ssem, rsem, axis, d):
    target = step(lax.axis_index(axis), 1 if d == 0 else 3)
    return pltpu.make_async_remote_copy(
        src_ref=st.at[d],
        dst_ref=r.at[d],
        send_sem=ssem.at[0, d],
        recv_sem=rsem.at[0, d],
        device_id={axis: target},
        device_id_type=MESH,
    )


def second_send(st, rb, ssem, rsem, axis, d):
    h = st.shape[1] // 2
    target = step(lax.axis_index(axis), 1 if d == 0 else 3)
    rows = pl.ds(d * h, h)
    return pltpu.make_async_remote_copy(
        src_ref=st.at[2, rows],
        dst_ref=rb.at[rows],
        send_sem=ssem.at[1, d],
        recv_sem=rsem.at[1, d],
        device_id={axis: target},
        device_id_type=MESH,
    )


def add_far(st, r):
    h = st.shape[1] // 2
    st[2, :h] = (st[2, :h].astype(F32) + r[0, :h].astype(F32)).astype(BF16)
    st[2, h:] = (st[2, h:].astype(F32) + r[1, h:].astype(F32)).astype(BF16)


def total_of(st, r, rb, lo, n):
    h = st.shape[1] // 2
    lanes = pl.ds(lo, n)
    top = st[3, :h, lanes].astype(F32) + r[1, :h, lanes].astype(F32) + rb[:h, lanes].astype(F32)
    low = st[3, h:, lanes].astype(F32) + r[0, h:, lanes].astype(F32) + rb[h:, lanes].astype(F32)
    return top.astype(BF16), low.astype(BF16)


def put(st, offset, lo, n, top, low):
    h = st.shape[1] // 2
    st[SLOT_A[offset], :h, lo : lo + n] = top
    st[SLOT_B[offset], h:, lo : lo + n] = low


def project_kernel(
    tok_hbm, gain_ref, w_hbm, kw_hbm, q_out, k_out, ssq_out,
    tok, xs, wbuf, kwbuf, st1, r1, r1b, st2, r2, r2b,
    kpart, kst1, kr1, kr1b, kst2, kr2, kr2b, kfin,
    ssq_own, ssq_in, ssq_sum, ssq_far,
    load_sem, w_sem, g_send, g_recv, s_send, s_recv, k_send, k_recv,
    a_send, a_recv, n_send, n_recv, d_send, d_recv, e_send, e_recv,
):
    x, z, y, core = (lax.axis_index(a) for a in (X, Z, Y, CORE))
    axes = (X, Z)
    barrier = pltpu.get_barrier_semaphore()
    for ox, oz in PEERS:
        pl.semaphore_signal(barrier, 1, device_id={X: step(x, ox), Z: step(z, oz)}, device_id_type=MESH)
    for by in (1, 3):
        pl.semaphore_signal(barrier, 1, device_id={Y: step(y, by)}, device_id_type=MESH)
    pl.semaphore_signal(barrier, 1, device_id={CORE: 1 - core}, device_id_type=MESH)

    def tok_load(p):
        return pltpu.make_async_copy(tok_hbm.at[pl.ds(p * R, R)], tok.at[p], load_sem.at[p])

    def w_load(ox, oz):
        col = (step(x, ox) * 4 + step(z, oz)) * 256
        return pltpu.make_async_copy(
            w_hbm.at[:, pl.ds(pl.multiple_of(col, 256), 256)], wbuf.at[ox * 4 + oz], w_sem.at[ox * 4 + oz]
        )

    kw_load = pltpu.make_async_copy(kw_hbm, kwbuf, load_sem.at[2])
    for p in range(2):
        tok_load(p).start()
    for ox in ORDER:
        for oz in ORDER:
            w_load(ox, oz).start()
    kw_load.start()

    def scale(p):
        xs[p] = (tok[p].astype(F32) * gain_ref[...].astype(F32)).astype(BF16)

    def gather(n, src, dst, by):
        return pltpu.make_async_remote_copy(
            src_ref=tok.at[src],
            dst_ref=tok.at[dst],
            send_sem=g_send.at[n],
            recv_sem=g_recv.at[n],
            device_id={Y: step(y, by)},
            device_id_type=MESH,
        )

    gathers = [
        gather(0, 0, 2, 1), gather(1, 1, 3, 3), gather(2, 1, 4, 1),
        gather(3, 0, 5, 3), gather(4, 2, 6, 1), gather(5, 3, 7, 3),
    ]
    for p in range(2):
        tok_load(p).wait()
    pl.semaphore_wait(barrier, len(PEERS) + 3)
    for n in range(4):
        gathers[n].start()
    for p in range(2):
        scale(p)

    def q_first(c, color, stage, d):
        st, r = (st1, r1) if stage == 0 else (st2, r2)
        axis = axes[color] if stage == 0 else axes[1 - color]
        return first_send(
            st.at[color, c], r.at[color, c], s_send.at[c, color, stage], s_recv.at[c, color, stage], axis, d
        )

    def q_second(c, color, stage, d):
        st, rb = (st1, r1b) if stage == 0 else (st2, r2b)
        axis = axes[color] if stage == 0 else axes[1 - color]
        return second_send(
            st.at[color, c], rb.at[color, c], s_send.at[c, color, stage], s_recv.at[c, color, stage], axis, d
        )

    def k_first(color, stage, d):
        st, r = (kst1, kr1) if stage == 0 else (kst2, kr2)
        axis = axes[color] if stage == 0 else axes[1 - color]
        return first_send(st.at[color], r.at[color], k_send.at[color, stage], k_recv.at[color, stage], axis, d)

    def k_second(color, stage, d):
        st, rb = (kst1, kr1b) if stage == 0 else (kst2, kr2b)
        axis = axes[color] if stage == 0 else axes[1 - color]
        return second_send(st.at[color], rb.at[color], k_send.at[color, stage], k_recv.at[color, stage], axis, d)

    mine = x * 4 + z
    k_off, k_half = piece_of(mine // 2)
    k_blk = step(y, k_off)
    k_slot = k_half * 2 + lax.rem(mine, 2)

    def key_send(n):
        ox, oz = PEERS[n]
        return pltpu.make_async_remote_copy(
            src_ref=kfin.at[step(x, ox) // 2],
            dst_ref=k_out.at[k_blk, core, k_slot],
            send_sem=a_send.at[n],
            recv_sem=a_recv.at[n],
            device_id={X: step(x, ox), Z: step(z, oz)},
            device_id_type=MESH,
        )

    def square_send(n):
        ox, oz = PEERS[n]
        return pltpu.make_async_remote_copy(
            src_ref=ssq_own,
            dst_ref=ssq_in.at[n],
            send_sem=n_send.at[n],
            recv_sem=n_recv.at[n],
            device_id={X: step(x, ox), Z: step(z, oz)},
            device_id_type=MESH,
        )

    def q_share(c):
        off, half = piece_of(c)
        part = q_out.at[step(y, off), core, half]
        return pltpu.make_async_remote_copy(
            src_ref=part,
            dst_ref=part,
            send_sem=d_send.at[c],
            recv_sem=d_recv.at[c],
            device_id={CORE: 1 - core},
            device_id_type=MESH,
        )

    k_share = pltpu.make_async_remote_copy(
        src_ref=k_out.at[:, core],
        dst_ref=k_out.at[:, core],
        send_sem=e_send.at[0],
        recv_sem=e_recv.at[0],
        device_id={CORE: 1 - core},
        device_id_type=MESH,
    )
    square_share = pltpu.make_async_remote_copy(
        src_ref=ssq_sum,
        dst_ref=ssq_far,
        send_sem=e_send.at[1],
        recv_sem=e_recv.at[1],
        device_id={CORE: 1 - core},
        device_id_type=MESH,
    )

    def put_squares(src, whose):
        for c in range(CH):
            off, half = piece_of(jnp.int32(c))
            row = step(y, off) * 4 + whose * 2 + half
            ssq_out[pl.ds(row, 1), :] = src[c : c + 1, :]

    both = [(color, d) for color in range(2) for d in range(2)]

    def body(i, carry):
        @pl.when(i == 2)
        def _():
            for n in range(2):
                gathers[n].wait_recv()
                gathers[4 + n].start()
            for p in (2, 3):
                scale(p)

        @pl.when(i == KI)
        def _():
            for n in range(2, 6):
                gathers[n].wait_recv()
            for p in range(4, 8):
                scale(p)

        @pl.when(i < CH)
        def _():
            lhs = xs[i]
            for n, ox in enumerate(ORDER):
                for oz in ORDER:
                    @pl.when(i == 0)
                    def _():
                        w_load(ox, oz).wait()

                    out = jnp.dot(lhs, wbuf[ox * 4 + oz], preferred_element_type=F32).astype(BF16)
                    h = R // 2
                    put(st1.at[0, i], ox, oz * HD, HD, out[:h, :HD], out[h:, :HD])
                    put(st1.at[1, i], oz, ox * HD, HD, out[:h, HD:], out[h:, HD:])
                if n == 1:
                    q_first(i, 0, 0, 0).start()
                if n == 2:
                    q_first(i, 0, 0, 1).start()
            for d in range(2):
                q_first(i, 1, 0, d).start()

        @pl.when(i == KI)
        def _():
            kw_load.wait()
            eye = lax.broadcasted_iota(jnp.int32, (R, R), 0) == lax.broadcasted_iota(jnp.int32, (R, R), 1)

            def one(p, carry):
                kpart[pl.ds(pl.multiple_of(p * R, R), R), :] = jnp.dot(
                    xs[p], kwbuf[...], preferred_element_type=F32
                ).astype(BF16)
                acc = jnp.zeros((R, 128), F32)
                for j in range(8):
                    t = tok[p, :, j * 128 : (j + 1) * 128].astype(F32)
                    acc = acc + t * t
                col = jnp.sum(acc, axis=1, keepdims=True)
                ssq_own[pl.ds(p, 1), :] = jnp.sum(jnp.where(eye, col, 0.0), axis=0, keepdims=True)
                return carry

            lax.fori_loop(0, CH, one, 0)
            for ox in range(4):
                for oz in range(4):
                    row = (step(x, ox) * 4 + step(z, oz)) * 64
                    rows = kpart[pl.ds(pl.multiple_of(row, 64), 64), :]
                    put(kst1.at[0], ox, oz * HD, HD, rows[:32, :HD], rows[32:, :HD])
                    put(kst1.at[1], oz, ox * HD, HD, rows[:32, HD:], rows[32:, HD:])
            for color, d in both:
                k_first(color, 0, d).start()
            for n in range(len(PEERS)):
                square_send(n).start()

        for stage in range(2):
            lag = 1 + 2 * stage

            @pl.when((i >= lag) & (i < CH + lag))
            def _(stage=stage, lag=lag):
                c = i - lag
                for color in range(2):
                    for d in range(2):
                        q_first(c, color, stage, d).wait_recv()
                    add_far((st1 if stage == 0 else st2).at[color, c], (r1 if stage == 0 else r2).at[color, c])
                    for d in range(2):
                        q_second(c, color, stage, d).start()

            @pl.when(i == KI + lag)
            def _(stage=stage):
                for color in range(2):
                    for d in range(2):
                        k_first(color, stage, d).wait_recv()
                    add_far((kst1 if stage == 0 else kst2).at[color], (kr1 if stage == 0 else kr2).at[color])
                    for d in range(2):
                        k_second(color, stage, d).start()

            if stage == 0:
                @pl.when((i >= 2) & (i < CH + 2))
                def _():
                    c = i - 2
                    for color in range(2):
                        for d in range(2):
                            q_second(c, color, 0, d).wait_recv()
                        for o in range(4):
                            top, low = total_of(st1.at[color, c], r1.at[color, c], r1b.at[color, c], o * HD, HD)
                            put(st2.at[color, c], o, 0, HD, top, low)
                        for d in range(2):
                            q_first(c, color, 1, d).start()

                @pl.when(i == KI + 2)
                def _():
                    for color in range(2):
                        for d in range(2):
                            k_second(color, 0, d).wait_recv()
                        for o in range(4):
                            top, low = total_of(kst1.at[color], kr1.at[color], kr1b.at[color], o * HD, HD)
                            put(kst2.at[color], o, 0, HD, top, low)
                        for d in range(2):
                            k_first(color, 1, d).start()

        @pl.when(i >= 4)
        def _():
            c = i - 4
            off, half = piece_of(c)
            blk = step(y, off)
            for color in range(2):
                for d in range(2):
                    q_second(c, color, 1, d).wait_recv()
                top, low = total_of(st2.at[color, c], r2.at[color, c], r2b.at[color, c], 0, HD)
                q_out[blk, core, half, color, : R // 2] = top
                q_out[blk, core, half, color, R // 2 :] = low
            q_share(c).start()

        @pl.when(i == KI + 4)
        def _():
            for color in range(2):
                for d in range(2):
                    k_second(color, 1, d).wait_recv()
                top, low = total_of(kst2.at[color], kr2.at[color], kr2b.at[color], 0, HD)
                kfin[color, :32] = top
                kfin[color, 32:] = low
            for n in range(len(PEERS)):
                key_send(n).start()
            k_out[k_blk, core, k_slot] = kfin[x // 2]
            total = ssq_own[...]
            for n in range(len(PEERS)):
                square_send(n).wait_recv()
                total = total + ssq_in[n]
            ssq_sum[...] = total
            square_share.start()
            put_squares(ssq_sum, core)

        @pl.when(i == KI + 6)
        def _():
            for n in range(len(PEERS)):
                key_send(n).wait_recv()
            k_share.start()

        return carry

    lax.fori_loop(0, LAST, body, 0)
    k_share.wait_recv()
    square_share.wait_recv()
    put_squares(ssq_far, 1 - core)

    def drain(c, carry):
        for color, d in both:
            for stage in range(2):
                q_first(c, color, stage, d).wait_send()
                q_second(c, color, stage, d).wait_send()
        q_share(c).wait()
        return carry

    for color, d in both:
        for stage in range(2):
            k_first(color, stage, d).wait_send()
            k_second(color, stage, d).wait_send()
    for copy in gathers:
        copy.wait_send()
    for n in range(len(PEERS)):
        key_send(n).wait_send()
        square_send(n).wait_send()
    k_share.wait_send()
    square_share.wait_send()
    lax.fori_loop(0, CH, drain, 0)


def project(tokens, gain, query_weight, key_weight):
    dma = pltpu.SemaphoreType.DMA
    vmem = pl.BlockSpec(memory_space=pltpu.VMEM)
    hbm = pl.BlockSpec(memory_space=pl.ANY)
    n = len(PEERS)
    k = tokens.shape[1]
    return pl.pallas_call(
        project_kernel,
        name="project",
        out_shape=(
            jax.ShapeDtypeStruct((4, 2, 2, 2, R, HD), BF16),
            jax.ShapeDtypeStruct((4, 2, 4, 64, HD), BF16),
            jax.ShapeDtypeStruct((16, 128), F32),
        ),
        in_specs=[hbm, vmem, hbm, hbm],
        out_specs=(vmem, vmem, vmem),
        scratch_shapes=[
            pltpu.VMEM((CH, R, k), BF16),
            pltpu.VMEM((CH, R, k), BF16),
            pltpu.VMEM((16, k, 256), BF16),
            pltpu.VMEM((k, 256), BF16),
            pltpu.VMEM((2, CH, 4, R, 512), BF16),
            pltpu.VMEM((2, CH, 2, R, 512), BF16),
            pltpu.VMEM((2, CH, R, 512), BF16),
            pltpu.VMEM((2, CH, 4, R, HD), BF16),
            pltpu.VMEM((2, CH, 2, R, HD), BF16),
            pltpu.VMEM((2, CH, R, HD), BF16),
            pltpu.VMEM((CH * R, 256), BF16),
            pltpu.VMEM((2, 4, 64, 512), BF16),
            pltpu.VMEM((2, 2, 64, 512), BF16),
            pltpu.VMEM((2, 64, 512), BF16),
            pltpu.VMEM((2, 4, 64, HD), BF16),
            pltpu.VMEM((2, 2, 64, HD), BF16),
            pltpu.VMEM((2, 64, HD), BF16),
            pltpu.VMEM((2, 64, HD), BF16),
            pltpu.VMEM((CH, 128), F32),
            pltpu.VMEM((n, CH, 128), F32),
            pltpu.VMEM((CH, 128), F32),
            pltpu.VMEM((CH, 128), F32),
            dma((3,)), dma((16,)), dma((6,)), dma((6,)),
            dma((CH, 2, 2, 2, 2)), dma((CH, 2, 2, 2, 2)),
            dma((2, 2, 2, 2)), dma((2, 2, 2, 2)),
            dma((n,)), dma((n,)), dma((n,)), dma((n,)),
            dma((CH,)), dma((CH,)), dma((2,)), dma((2,)),
        ],
        compiler_params=pltpu.CompilerParams(
            collective_id=0, has_side_effects=True, vmem_limit_bytes=56 * 1024 * 1024
        ),
    )(tokens, gain, query_weight, key_weight)


QB = 128
KB = 256
WIN = 384
QWIN = 144
OWN = NS // 2
SCALE = math.log2(math.e) / math.sqrt(HD)
NT = (((1,), (1,)), ((), ()))


def attention_kernel(
    q_ref, k_ref, ssq_ref, tab_ref, doc_ref, span_ref, span_smem, out_hbm,
    keys, marks, qs, sbuf, km, tot, cnt, obuf, sem,
):
    core = lax.axis_index(CORE)
    docs = doc_ref[...]
    spans = span_ref[...]

    def below(a, v):
        return jnp.sum(jnp.where(a < v, 1.0, 0.0)).astype(jnp.int32)

    c1, c2, c3 = below(docs, 1), below(docs, 2), below(docs, 3)
    mid = below(spans, OWN)
    eye = lax.broadcasted_iota(jnp.int32, (QB, QB), 0) == lax.broadcasted_iota(jnp.int32, (QB, QB), 1)
    low_lanes = lax.broadcasted_iota(jnp.int32, (QB, HD), 1) < HD // 2

    def start_of(i):
        return jnp.where(i >= c3, c3, jnp.where(i >= c2, c2, jnp.where(i >= c1, c1, 0)))

    def tables(b):
        t = tab_ref[pl.ds(pl.multiple_of(b * QB, QB), QB), :]
        turned = pltpu.roll(t, HD // 2, 1)
        row = lax.rsqrt(ssq_ref[pl.ds(b, 1), :] / D + 1e-05)
        col = jnp.sum(jnp.where(eye, row, 0.0), axis=1, keepdims=True)
        return jnp.where(low_lanes, t, turned) * col, jnp.where(low_lanes, -turned, t) * col

    def turn(v, cosine, sine):
        return v * cosine + pltpu.roll(v, HD // 2, 1) * sine

    def make_keys(b, carry):
        cosine, sine = tables(b)
        rows = pl.ds(pl.multiple_of(b * QB, QB), QB)
        keys[rows, :] = turn(k_ref[rows, :].astype(F32), cosine, sine).astype(BF16)
        return carry

    lax.fori_loop(0, TOKENS // QB, make_keys, 0)

    def base_of(kb):
        return span_smem[kb * KB] // 128 * 128

    def make_marks(kb, carry):
        ids = lax.broadcasted_iota(jnp.int32, (WIN, 128), 0) + base_of(kb)
        for half in range(2):
            row = span_ref[pl.ds(kb * 2 + half, 1), :]
            marks[kb, :, half * 128 : (half + 1) * 128] = jnp.where(ids == row, 1.0, 0.0).astype(BF16)
        return carry

    lax.fori_loop(0, TOKENS // KB, make_marks, 0)
    tot[...] = jnp.zeros_like(tot)
    cnt[...] = jnp.zeros_like(cnt)
    ones = jnp.ones((QB, 128), BF16)

    def block(qb, carry):
        cosine, sine = tables(qb)
        for h in range(2):
            v = q_ref[qb, h * QB : (h + 1) * QB, :].astype(F32)
            qs[h * QB : (h + 1) * QB, :] = (turn(v, cosine, sine) * SCALE).astype(BF16)
        first = qb * QB
        kb0 = start_of(first) // KB
        kb1 = qb // 2
        rows = lax.broadcasted_iota(jnp.int32, (QB, 1), 0) + first
        begin = start_of(rows)
        query = qs[...]

        def score(kb, peak):
            block_keys = keys[pl.ds(pl.multiple_of(kb * KB, KB), KB), :]
            s = lax.dot_general(query, block_keys, NT, preferred_element_type=F32)
            cols = lax.broadcasted_iota(jnp.int32, (QB, KB), 1) + kb * KB
            seen = (cols <= rows) & (cols >= begin)
            s0 = jnp.where(seen, s[:QB], -1e30)
            s1 = jnp.where(seen, s[QB:], -1e30)
            sbuf[kb - kb0, :QB, :] = s0
            sbuf[kb - kb0, QB:, :] = s1
            top = jnp.concatenate([jnp.maximum(s0[:, :128], s0[:, 128:]), jnp.maximum(s1[:, :128], s1[:, 128:])], 0)
            return jnp.maximum(peak, top)

        peak = lax.fori_loop(kb0, kb1 + 1, score, jnp.full((2 * QB, 128), -1e30, F32))
        peak = jnp.max(peak, axis=1, keepdims=True)
        km[...] = jnp.zeros_like(km)

        def mass(kb, total):
            e = jnp.exp2(sbuf[kb - kb0] - peak)
            got = lax.dot_general(e.astype(BF16), marks[kb], NT, preferred_element_type=F32)
            lanes = pl.ds(pl.multiple_of(base_of(kb), 128), WIN)
            km[:, lanes] = km[:, lanes] + got
            return total + e[:, :128] + e[:, 128:]

        total = lax.fori_loop(kb0, kb1 + 1, mass, jnp.zeros((2 * QB, 128), F32))
        scale = 1.0 / jnp.sum(total, axis=1, keepdims=True)
        lead = jnp.maximum(span_smem[first] - core * OWN, 0) // 8 * 8
        ids = lax.broadcasted_iota(jnp.int32, (QWIN, QB), 0) + lead
        row = span_ref[pl.ds(qb, 1), :] - core * OWN
        pick = jnp.where(ids == row, 1.0, 0.0).astype(BF16)
        at = pl.ds(pl.multiple_of(lead, 8), QWIN)
        for h in range(2):
            for j in range(4):
                lanes = slice(j * 256, (j + 1) * 256)
                part = (km[h * QB : (h + 1) * QB, lanes] * scale[h * QB : (h + 1) * QB]).astype(BF16)
                tot[h, at, lanes] = tot[h, at, lanes] + jnp.dot(pick, part, preferred_element_type=F32)
        cnt[at, :] = cnt[at, :] + jnp.dot(pick, ones, preferred_element_type=F32)
        return carry

    lo = core * mid // QB
    hi = jnp.where(core == 0, (mid + QB - 1) // QB, TOKENS // QB)
    lax.fori_loop(lo, hi, block, 0)

    step_rows = 64

    def out_copy(n):
        rows = pl.ds(n * step_rows, step_rows)
        return pltpu.make_async_copy(obuf.at[rows], out_hbm.at[rows], sem.at[n])

    for n in range(OWN // step_rows):
        rows = slice(n * step_rows, (n + 1) * step_rows)
        share = 1.0 / cnt[rows, :]
        for h in range(2):
            for j in range(NS // 128):
                lanes = slice(j * 128, (j + 1) * 128)
                obuf[rows, h, lanes] = jnp.log(tot[h, rows, lanes] * share + 1e-06)
        out_copy(n).start()
    for n in range(OWN // step_rows):
        out_copy(n).wait()


def attention(q, k, ssq, table, documents, span_ids):
    vmem = pl.BlockSpec(memory_space=pltpu.VMEM)
    return pl.pallas_call(
        attention_kernel,
        name="attention",
        out_shape=jax.ShapeDtypeStruct((OWN, 2, NS), F32),
        in_specs=[vmem] * 6 + [pl.BlockSpec(memory_space=pltpu.SMEM)],
        out_specs=pl.BlockSpec(memory_space=pl.ANY),
        scratch_shapes=[
            pltpu.VMEM((TOKENS, HD), BF16),
            pltpu.VMEM((TOKENS // KB, WIN, KB), BF16),
            pltpu.VMEM((2 * QB, HD), BF16),
            pltpu.VMEM((6, 2 * QB, KB), F32),
            pltpu.VMEM((2 * QB, NS + 256), F32),
            pltpu.VMEM((2, OWN + QWIN, NS), F32),
            pltpu.VMEM((OWN + QWIN, 128), F32),
            pltpu.VMEM((OWN, 2, NS), F32),
            pltpu.SemaphoreType.DMA((8,)),
        ],
        compiler_params=pltpu.CompilerParams(vmem_limit_bytes=40 * 1024 * 1024),
    )(q, k, ssq, table, documents.reshape(16, 128), span_ids.reshape(16, 128), span_ids)


def angle_table():
    i = np.arange(HD // 2, dtype=np.float64)
    f = 500000.0 ** (-i / (HD // 2))
    w = 2.0 * np.pi / f
    s = (8192.0 / w - 1.0) / 3.0
    f = np.where(w < 2048.0, f, np.where(w > 8192.0, f / 8.0, (1.0 - s) * f / 8.0 + s * f))
    phase = np.arange(TOKENS, dtype=np.float64)[:, None] * f[None, :]
    return np.concatenate([np.cos(phase), np.sin(phase)], axis=1).astype(np.float32)


def local(tokens, norm_gain, query_weight, key_weight, documents, span_ids):
    q, k, ssq = project(tokens, norm_gain.reshape(1, -1), query_weight, key_weight)
    table = jnp.asarray(angle_table())
    return attention(
        q.reshape(16, 2 * QB, HD), k.reshape(TOKENS, HD), ssq, table, documents, span_ids
    )


def solution(mesh):
    finer = Mesh(
        mesh.devices.reshape(mesh.shape["blk"], 4, 4, mesh.shape["kv"]),
        (Y, X, Z, CORE),
    )
    return jax.shard_map(
        local,
        mesh=finer,
        in_specs=(P((Y, CORE), MP), P(MP), P(MP, Y), P(MP, Y), P(), P()),
        out_specs=P(CORE, BLK_MP, None),
        check_vma=False,
    )
```

```python
import functools
import math

import jax
import jax.numpy as jnp
import numpy as np
from jax import lax
from jax.experimental import pallas as pl
from jax.experimental.pallas import tpu as pltpu
from jax.sharding import Mesh
from jax.sharding import PartitionSpec as P

D = 16384
HD = 128
TOKENS = 2048
NS = 1024
X, Z, Y, CORE = "mp_0", "mp_1", "blk", "kv"
MP = (X, Z)
BLK_MP = (Y, X, Z)
MESH = pl.DeviceIdType.MESH
F32 = jnp.float32
BF16 = jnp.bfloat16
RING = 4
CH = 8
R = 128
KI = 4
LAST = CH + 4
WS = 8
SLOT_A = {2: 0, 1: 2, 3: 1, 0: 3}
SLOT_B = {2: 1, 1: 0, 3: 2, 0: 3}
ORDER = (2, 1, 3, 0)
PEERS = [(ox, oz) for ox in range(4) for oz in range(4) if (ox, oz) != (0, 0)]


def step(pos, by):
    return lax.rem(pos + by, RING)


def piece_of(i):
    half = lax.rem(i + i // 4 + i // 6, 2)
    far = i // 6
    other = (i + 4) // 6
    offset = other * (1 - far) * (3 - 2 * lax.rem(i, 2)) + 2 * far
    return offset, half


def first_send(st, r, ssem, rsem, axis, d):
    target = step(lax.axis_index(axis), 1 if d == 0 else 3)
    return pltpu.make_async_remote_copy(
        src_ref=st.at[d],
        dst_ref=r.at[d],
        send_sem=ssem.at[0, d],
        recv_sem=rsem.at[0, d],
        device_id={axis: target},
        device_id_type=MESH,
    )


def second_send(st, rb, ssem, rsem, axis, d):
    h = st.shape[1] // 2
    target = step(lax.axis_index(axis), 1 if d == 0 else 3)
    rows = pl.ds(d * h, h)
    return pltpu.make_async_remote_copy(
        src_ref=st.at[2, rows],
        dst_ref=rb.at[rows],
        send_sem=ssem.at[1, d],
        recv_sem=rsem.at[1, d],
        device_id={axis: target},
        device_id_type=MESH,
    )


def add_far(st, r):
    h = st.shape[1] // 2
    st[2, :h] = (st[2, :h].astype(F32) + r[0, :h].astype(F32)).astype(BF16)
    st[2, h:] = (st[2, h:].astype(F32) + r[1, h:].astype(F32)).astype(BF16)


def total_of(st, r, rb, lo, n):
    h = st.shape[1] // 2
    lanes = pl.ds(lo, n)
    top = st[3, :h, lanes].astype(F32) + r[1, :h, lanes].astype(F32) + rb[:h, lanes].astype(F32)
    low = st[3, h:, lanes].astype(F32) + r[0, h:, lanes].astype(F32) + rb[h:, lanes].astype(F32)
    return top.astype(BF16), low.astype(BF16)


def put(st, offset, lo, n, top, low):
    h = st.shape[1] // 2
    st[SLOT_A[offset], :h, lo : lo + n] = top
    st[SLOT_B[offset], h:, lo : lo + n] = low


def project_kernel(
    tok_hbm, gain_ref, w_hbm, kw_hbm, q_out, k_out, ssq_out,
    tok, xs, wbuf, kwbuf, st1, r1, r1b, st2, r2, r2b,
    kpart, kst1, kr1, kr1b, kst2, kr2, kr2b, kfin,
    ssq_own, ssq_in, ssq_sum, ssq_far,
    load_sem, w_sem, g_send, g_recv, s_send, s_recv, k_send, k_recv,
    a_send, a_recv, n_send, n_recv, d_send, d_recv, e_send, e_recv,
):
    x, z, y, core = (lax.axis_index(a) for a in (X, Z, Y, CORE))
    axes = (X, Z)
    barrier = pltpu.get_barrier_semaphore()
    for ox, oz in PEERS:
        pl.semaphore_signal(barrier, 1, device_id={X: step(x, ox), Z: step(z, oz)}, device_id_type=MESH)
    for by in (1, 3):
        pl.semaphore_signal(barrier, 1, device_id={Y: step(y, by)}, device_id_type=MESH)
    pl.semaphore_signal(barrier, 1, device_id={CORE: 1 - core}, device_id_type=MESH)

    def tok_load(p):
        return pltpu.make_async_copy(tok_hbm.at[pl.ds(p * R, R)], tok.at[p], load_sem.at[p])

    slab = w_hbm.shape[0] // WS

    def w_load(n):
        rows = pl.ds(n * slab, slab)
        return pltpu.make_async_copy(w_hbm.at[rows], wbuf.at[rows], w_sem.at[n])

    kw_load = pltpu.make_async_copy(kw_hbm, kwbuf, load_sem.at[2])
    for p in range(2):
        tok_load(p).start()
    for n in range(WS):
        w_load(n).start()
    kw_load.start()

    def scale(p):
        xs[p * R : (p + 1) * R] = (tok[p].astype(F32) * gain_ref[...].astype(F32)).astype(BF16)

    def gather(n, src, dst, by):
        return pltpu.make_async_remote_copy(
            src_ref=tok.at[src],
            dst_ref=tok.at[dst],
            send_sem=g_send.at[n],
            recv_sem=g_recv.at[n],
            device_id={Y: step(y, by)},
            device_id_type=MESH,
        )

    gathers = [
        gather(0, 0, 2, 1), gather(1, 1, 3, 3), gather(2, 1, 4, 1),
        gather(3, 0, 5, 3), gather(4, 2, 6, 1), gather(5, 3, 7, 3),
    ]
    for p in range(2):
        tok_load(p).wait()
    pl.semaphore_wait(barrier, len(PEERS) + 3)
    for n in range(4):
        gathers[n].start()
    for p in range(2):
        scale(p)

    def q_first(c, color, stage, d):
        st, r = (st1, r1) if stage == 0 else (st2, r2)
        axis = axes[color] if stage == 0 else axes[1 - color]
        return first_send(
            st.at[color, c], r.at[color, c], s_send.at[c, color, stage], s_recv.at[c, color, stage], axis, d
        )

    def q_second(c, color, stage, d):
        st, rb = (st1, r1b) if stage == 0 else (st2, r2b)
        axis = axes[color] if stage == 0 else axes[1 - color]
        return second_send(
            st.at[color, c], rb.at[color, c], s_send.at[c, color, stage], s_recv.at[c, color, stage], axis, d
        )

    def k_first(color, stage, d):
        st, r = (kst1, kr1) if stage == 0 else (kst2, kr2)
        axis = axes[color] if stage == 0 else axes[1 - color]
        return first_send(st.at[color], r.at[color], k_send.at[color, stage], k_recv.at[color, stage], axis, d)

    def k_second(color, stage, d):
        st, rb = (kst1, kr1b) if stage == 0 else (kst2, kr2b)
        axis = axes[color] if stage == 0 else axes[1 - color]
        return second_send(st.at[color], rb.at[color], k_send.at[color, stage], k_recv.at[color, stage], axis, d)

    mine = x * 4 + z
    k_off, k_half = piece_of(mine // 2)
    k_blk = step(y, k_off)
    k_slot = k_half * 2 + lax.rem(mine, 2)

    def key_send(n):
        ox, oz = PEERS[n]
        return pltpu.make_async_remote_copy(
            src_ref=kfin.at[step(x, ox) // 2],
            dst_ref=k_out.at[k_blk, core, k_slot],
            send_sem=a_send.at[n],
            recv_sem=a_recv.at[n],
            device_id={X: step(x, ox), Z: step(z, oz)},
            device_id_type=MESH,
        )

    def square_send(n):
        ox, oz = PEERS[n]
        return pltpu.make_async_remote_copy(
            src_ref=ssq_own,
            dst_ref=ssq_in.at[n],
            send_sem=n_send.at[n],
            recv_sem=n_recv.at[n],
            device_id={X: step(x, ox), Z: step(z, oz)},
            device_id_type=MESH,
        )

    def q_share(c):
        off, half = piece_of(c)
        part = q_out.at[step(y, off), core, half]
        return pltpu.make_async_remote_copy(
            src_ref=part,
            dst_ref=part,
            send_sem=d_send.at[c],
            recv_sem=d_recv.at[c],
            device_id={CORE: 1 - core},
            device_id_type=MESH,
        )

    k_share = pltpu.make_async_remote_copy(
        src_ref=k_out.at[:, core],
        dst_ref=k_out.at[:, core],
        send_sem=e_send.at[0],
        recv_sem=e_recv.at[0],
        device_id={CORE: 1 - core},
        device_id_type=MESH,
    )
    square_share = pltpu.make_async_remote_copy(
        src_ref=ssq_sum,
        dst_ref=ssq_far,
        send_sem=e_send.at[1],
        recv_sem=e_recv.at[1],
        device_id={CORE: 1 - core},
        device_id_type=MESH,
    )

    def put_squares(src, whose):
        for c in range(CH):
            off, half = piece_of(jnp.int32(c))
            row = step(y, off) * 4 + whose * 2 + half
            ssq_out[pl.ds(row, 1), :] = src[c : c + 1, :]

    both = [(color, d) for color in range(2) for d in range(2)]

    def body(i, carry):
        @pl.when(i == 2)
        def _():
            for n in range(2):
                gathers[n].wait_recv()
                gathers[4 + n].start()
            for p in (2, 3):
                scale(p)

        @pl.when(i == KI)
        def _():
            for n in range(2, 6):
                gathers[n].wait_recv()
            for p in range(4, 8):
                scale(p)

        @pl.when(i == 0)
        def _():
            for n in range(WS):
                w_load(n).wait()

        @pl.when((i < CH) & (lax.rem(i, 2) == 0))
        def _():
            lhs = xs[pl.ds(pl.multiple_of(i * R, 2 * R), 2 * R), :]
            for n, ox in enumerate(ORDER):
                for oz in ORDER:
                    col = pl.multiple_of((step(x, ox) * 4 + step(z, oz)) * 256, 256)
                    out = jnp.dot(lhs, wbuf[:, pl.ds(col, 256)], preferred_element_type=F32).astype(BF16)
                    for u in range(2):
                        a, b, e = u * R, u * R + R // 2, u * R + R
                        put(st1.at[0, i + u], ox, oz * HD, HD, out[a:b, :HD], out[b:e, :HD])
                        put(st1.at[1, i + u], oz, ox * HD, HD, out[a:b, HD:], out[b:e, HD:])
                if n == 1:
                    q_first(i, 0, 0, 0).start()
                if n == 2:
                    q_first(i, 0, 0, 1).start()
            for d in range(2):
                q_first(i, 1, 0, d).start()
            for color, d in both:
                q_first(i + 1, color, 0, d).start()

        def key_part(lo, hi):
            eye = lax.broadcasted_iota(jnp.int32, (R, R), 0) == lax.broadcasted_iota(jnp.int32, (R, R), 1)

            def one(p, carry):
                kpart[pl.ds(pl.multiple_of(p * R, R), R), :] = jnp.dot(
                    xs[pl.ds(pl.multiple_of(p * R, R), R), :], kwbuf[...], preferred_element_type=F32
                ).astype(BF16)
                acc = jnp.zeros((R, 128), F32)
                for j in range(8):
                    t = tok[p, :, j * 128 : (j + 1) * 128].astype(F32)
                    acc = acc + t * t
                col = jnp.sum(acc, axis=1, keepdims=True)
                ssq_own[pl.ds(p, 1), :] = jnp.sum(jnp.where(eye, col, 0.0), axis=0, keepdims=True)
                return carry

            lax.fori_loop(lo, hi, one, 0)

        @pl.when(i == 1)
        def _():
            kw_load.wait()
            key_part(0, 2)

        @pl.when(i == 3)
        def _():
            key_part(2, 4)

        @pl.when(i == KI)
        def _():
            key_part(4, CH)
            for ox in range(4):
                for oz in range(4):
                    row = (step(x, ox) * 4 + step(z, oz)) * 64
                    rows = kpart[pl.ds(pl.multiple_of(row, 64), 64), :]
                    put(kst1.at[0], ox, oz * HD, HD, rows[:32, :HD], rows[32:, :HD])
                    put(kst1.at[1], oz, ox * HD, HD, rows[:32, HD:], rows[32:, HD:])
            for color, d in both:
                k_first(color, 0, d).start()
            for n in range(len(PEERS)):
                square_send(n).start()

        for stage in range(2):
            lag = 1 + 2 * stage

            @pl.when((i >= lag) & (i < CH + lag))
            def _(stage=stage, lag=lag):
                c = i - lag
                for color in range(2):
                    for d in range(2):
                        q_first(c, color, stage, d).wait_recv()
                    add_far((st1 if stage == 0 else st2).at[color, c], (r1 if stage == 0 else r2).at[color, c])
                    for d in range(2):
                        q_second(c, color, stage, d).start()

            @pl.when(i == KI + lag)
            def _(stage=stage):
                for color in range(2):
                    for d in range(2):
                        k_first(color, stage, d).wait_recv()
                    add_far((kst1 if stage == 0 else kst2).at[color], (kr1 if stage == 0 else kr2).at[color])
                    for d in range(2):
                        k_second(color, stage, d).start()

            if stage == 0:
                @pl.when((i >= 2) & (i < CH + 2))
                def _():
                    c = i - 2
                    for color in range(2):
                        for d in range(2):
                            q_second(c, color, 0, d).wait_recv()
                        for o in range(4):
                            top, low = total_of(st1.at[color, c], r1.at[color, c], r1b.at[color, c], o * HD, HD)
                            put(st2.at[color, c], o, 0, HD, top, low)
                        for d in range(2):
                            q_first(c, color, 1, d).start()

                @pl.when(i == KI + 2)
                def _():
                    for color in range(2):
                        for d in range(2):
                            k_second(color, 0, d).wait_recv()
                        for o in range(4):
                            top, low = total_of(kst1.at[color], kr1.at[color], kr1b.at[color], o * HD, HD)
                            put(kst2.at[color], o, 0, HD, top, low)
                        for d in range(2):
                            k_first(color, 1, d).start()

        @pl.when(i >= 4)
        def _():
            c = i - 4
            off, half = piece_of(c)
            blk = step(y, off)
            for color in range(2):
                for d in range(2):
                    q_second(c, color, 1, d).wait_recv()
                top, low = total_of(st2.at[color, c], r2.at[color, c], r2b.at[color, c], 0, HD)
                q_out[blk, core, half, color, : R // 2] = top
                q_out[blk, core, half, color, R // 2 :] = low
            q_share(c).start()

        @pl.when(i == KI + 4)
        def _():
            for color in range(2):
                for d in range(2):
                    k_second(color, 1, d).wait_recv()
                top, low = total_of(kst2.at[color], kr2.at[color], kr2b.at[color], 0, HD)
                kfin[color, :32] = top
                kfin[color, 32:] = low
            for n in range(len(PEERS)):
                key_send(n).start()
            k_out[k_blk, core, k_slot] = kfin[x // 2]
            total = ssq_own[...]
            for n in range(len(PEERS)):
                square_send(n).wait_recv()
                total = total + ssq_in[n]
            ssq_sum[...] = total
            square_share.start()
            put_squares(ssq_sum, core)

        @pl.when(i == KI + 6)
        def _():
            for n in range(len(PEERS)):
                key_send(n).wait_recv()
            k_share.start()

        return carry

    lax.fori_loop(0, LAST, body, 0)
    k_share.wait_recv()
    square_share.wait_recv()
    put_squares(ssq_far, 1 - core)

    def drain(c, carry):
        for color, d in both:
            for stage in range(2):
                q_first(c, color, stage, d).wait_send()
                q_second(c, color, stage, d).wait_send()
        q_share(c).wait()
        return carry

    for color, d in both:
        for stage in range(2):
            k_first(color, stage, d).wait_send()
            k_second(color, stage, d).wait_send()
    for copy in gathers:
        copy.wait_send()
    for n in range(len(PEERS)):
        key_send(n).wait_send()
        square_send(n).wait_send()
    k_share.wait_send()
    square_share.wait_send()
    lax.fori_loop(0, CH, drain, 0)


def project(tokens, gain, query_weight, key_weight):
    dma = pltpu.SemaphoreType.DMA
    vmem = pl.BlockSpec(memory_space=pltpu.VMEM)
    hbm = pl.BlockSpec(memory_space=pltpu.HBM)
    n = len(PEERS)
    k = tokens.shape[1]
    return pl.pallas_call(
        project_kernel,
        name="project",
        out_shape=(
            jax.ShapeDtypeStruct((4, 2, 2, 2, R, HD), BF16),
            jax.ShapeDtypeStruct((4, 2, 4, 64, HD), BF16),
            jax.ShapeDtypeStruct((16, 128), F32),
        ),
        in_specs=[hbm, vmem, hbm, hbm],
        out_specs=(vmem, vmem, vmem),
        scratch_shapes=[
            pltpu.VMEM((CH, R, k), BF16),
            pltpu.VMEM((CH * R, k), BF16),
            pltpu.VMEM((k, query_weight.shape[1]), BF16),
            pltpu.VMEM((k, 256), BF16),
            pltpu.VMEM((2, CH, 4, R, 512), BF16),
            pltpu.VMEM((2, CH, 2, R, 512), BF16),
            pltpu.VMEM((2, CH, R, 512), BF16),
            pltpu.VMEM((2, CH, 4, R, HD), BF16),
            pltpu.VMEM((2, CH, 2, R, HD), BF16),
            pltpu.VMEM((2, CH, R, HD), BF16),
            pltpu.VMEM((CH * R, 256), BF16),
            pltpu.VMEM((2, 4, 64, 512), BF16),
            pltpu.VMEM((2, 2, 64, 512), BF16),
            pltpu.VMEM((2, 64, 512), BF16),
            pltpu.VMEM((2, 4, 64, HD), BF16),
            pltpu.VMEM((2, 2, 64, HD), BF16),
            pltpu.VMEM((2, 64, HD), BF16),
            pltpu.VMEM((2, 64, HD), BF16),
            pltpu.VMEM((CH, 128), F32),
            pltpu.VMEM((n, CH, 128), F32),
            pltpu.VMEM((CH, 128), F32),
            pltpu.VMEM((CH, 128), F32),
            dma((3,)), dma((WS,)), dma((6,)), dma((6,)),
            dma((CH, 2, 2, 2, 2)), dma((CH, 2, 2, 2, 2)),
            dma((2, 2, 2, 2)), dma((2, 2, 2, 2)),
            dma((n,)), dma((n,)), dma((n,)), dma((n,)),
            dma((CH,)), dma((CH,)), dma((2,)), dma((2,)),
        ],
        compiler_params=pltpu.CompilerParams(
            collective_id=0, has_side_effects=True, vmem_limit_bytes=54 * 1024 * 1024
        ),
    )(tokens, gain, query_weight, key_weight)


SUB = 128
QB = 256
KB = 256
WIN = 384
PARTS = ((0, 144), (144, 128))
OWN = NS // 2
GROUP = 64
SCALE = math.log2(math.e) / math.sqrt(HD)
NT = (((1,), (1,)), ((), ()))


def attention_kernel(
    q_ref, k_ref, ssq_ref, tab_ref, doc_ref, span_ref, span_smem, out_hbm,
    keys, marks, qs, sbuf, peaks, sums, km, tot, cnt, obuf, sem,
):
    core = lax.axis_index(CORE)
    docs = doc_ref[...]
    spans = span_ref[...]

    def below(a, v):
        return jnp.sum(jnp.where(a < v, 1.0, 0.0)).astype(jnp.int32)

    c1, c2, c3 = below(docs, 1), below(docs, 2), below(docs, 3)
    mid = below(spans, OWN)
    lo = core * mid // QB
    hi = jnp.where(core == 0, (mid + QB - 1) // QB, TOKENS // QB)
    eye = lax.broadcasted_iota(jnp.int32, (SUB, SUB), 0) == lax.broadcasted_iota(jnp.int32, (SUB, SUB), 1)
    low_lanes = lax.broadcasted_iota(jnp.int32, (SUB, HD), 1) < HD // 2

    def start_of(i):
        return jnp.where(i >= c3, c3, jnp.where(i >= c2, c2, jnp.where(i >= c1, c1, 0)))

    def tables(b):
        t = tab_ref[pl.ds(pl.multiple_of(b * SUB, SUB), SUB), :]
        turned = pltpu.roll(t, HD // 2, 1)
        row = lax.rsqrt(ssq_ref[pl.ds(b, 1), :] / D + 1e-05)
        col = jnp.sum(jnp.where(eye, row, 0.0), axis=1, keepdims=True)
        return jnp.where(low_lanes, t, turned) * col, jnp.where(low_lanes, -turned, t) * col

    def turn(v, cosine, sine):
        return v * cosine + pltpu.roll(v, HD // 2, 1) * sine

    def base_of(kb):
        return span_smem[kb * KB] // 128 * 128

    def prepare(kb, carry):
        ids = lax.broadcasted_iota(jnp.int32, (WIN, 128), 0) + base_of(kb)
        for half in range(2):
            b = kb * 2 + half
            cosine, sine = tables(b)
            rows = pl.ds(pl.multiple_of(b * SUB, SUB), SUB)
            keys[rows, :] = turn(k_ref[rows, :].astype(F32), cosine, sine).astype(BF16)
            row = span_ref[pl.ds(b, 1), :]
            marks[kb, :, half * 128 : (half + 1) * 128] = jnp.where(ids == row, 1.0, 0.0).astype(BF16)
        return carry

    lax.fori_loop(start_of(lo * QB) // KB, hi, prepare, 0)
    tot[...] = jnp.zeros_like(tot)
    cnt[...] = jnp.zeros_like(cnt)
    ones = jnp.ones((QB, 128), BF16)

    def out_copy(n):
        rows = pl.ds(pl.multiple_of(n * GROUP, GROUP), GROUP)
        return pltpu.make_async_copy(obuf.at[rows], out_hbm.at[rows], sem.at[n])

    def finish(n, carry):
        rows = pl.ds(pl.multiple_of(n * GROUP, GROUP), GROUP)
        share = 1.0 / cnt[rows, :]
        for h in range(2):
            for j in range(NS // 128):
                lanes = slice(j * 128, (j + 1) * 128)
                obuf[rows, h, lanes] = jnp.log(tot[h, rows, lanes] * share + 1e-06)
        out_copy(n).start()
        return carry

    def block(qb, done):
        first = qb * QB
        for u in range(2):
            cosine, sine = tables(qb * 2 + u)
            for h in range(2):
                v = q_ref[qb * 2 + u, h * SUB : (h + 1) * SUB, :].astype(F32)
                at = h * QB + u * SUB
                qs[at : at + SUB, :] = (turn(v, cosine, sine) * SCALE).astype(BF16)
        kb0 = start_of(first) // KB
        last = span_smem[first + QB - 1]
        tile0 = base_of(kb0) // 256

        peaks[...] = jnp.full_like(peaks, -1e30)

        def score(kb, carry):
            block_keys = keys[pl.ds(pl.multiple_of(kb * KB, KB), KB), :]
            s = lax.dot_general(qs[...], block_keys, NT, preferred_element_type=F32)
            cols = lax.broadcasted_iota(jnp.int32, (SUB, KB), 1) + kb * KB
            for u in range(2):
                rows = lax.broadcasted_iota(jnp.int32, (SUB, 1), 0) + (first + u * SUB)
                seen = (cols <= rows) & (cols >= start_of(rows))
                for h in range(2):
                    at = slice(h * QB + u * SUB, h * QB + (u + 1) * SUB)
                    part = jnp.where(seen, s[at], -1e30)
                    sbuf[kb - kb0, at, :] = part
                    peaks[at, :] = jnp.maximum(peaks[at, :], jnp.maximum(part[:, :128], part[:, 128:]))
            return carry

        lax.fori_loop(kb0, qb + 1, score, 0)
        peak = jnp.max(peaks[...], axis=1, keepdims=True)
        sums[...] = jnp.zeros_like(sums)

        def clear(t, carry):
            km[:, pl.ds(pl.multiple_of(t * 256, 256), 256)] = jnp.zeros((2 * QB, 256), F32)
            return carry

        lax.fori_loop(tile0, jnp.maximum(base_of(qb) + WIN - 1, last) // 256 + 1, clear, 0)

        def mass(kb, carry):
            e = jnp.exp2(sbuf[kb - kb0] - peak)
            sums[...] = sums[...] + e[:, :128] + e[:, 128:]
            got = lax.dot_general(e.astype(BF16), marks[kb], NT, preferred_element_type=F32)
            lanes = pl.ds(pl.multiple_of(base_of(kb), 128), WIN)
            km[:, lanes] = km[:, lanes] + got
            return carry

        lax.fori_loop(kb0, qb + 1, mass, 0)
        scale = 1.0 / jnp.sum(sums[...], axis=1, keepdims=True)
        lead = jnp.maximum(span_smem[first] - core * OWN, 0) // 8 * 8
        row = jnp.concatenate([span_ref[pl.ds(qb * 2, 1), :], span_ref[pl.ds(qb * 2 + 1, 1), :]], axis=1)

        def gather_part(lo_row, n):
            ids = lax.broadcasted_iota(jnp.int32, (n, QB), 0) + (lead + lo_row + core * OWN)
            pick = jnp.where(ids == row, 1.0, 0.0).astype(BF16)
            at = pl.ds(pl.multiple_of(lead + lo_row, 8), n)

            def tile(t, carry):
                lanes = pl.ds(pl.multiple_of(t * 256, 256), 256)
                for h in range(2):
                    hs = slice(h * QB, (h + 1) * QB)
                    part = (km[hs, lanes] * scale[hs]).astype(BF16)
                    tot[h, at, lanes] = tot[h, at, lanes] + jnp.dot(pick, part, preferred_element_type=F32)
                return carry

            lax.fori_loop(tile0, last // 256 + 1, tile, 0)
            cnt[at, :] = cnt[at, :] + jnp.dot(pick, ones, preferred_element_type=F32)

        gather_part(*PARTS[0])

        @pl.when(last - core * OWN >= lead + PARTS[1][0])
        def _():
            gather_part(*PARTS[1])

        ready = (span_smem[jnp.minimum(first + QB, TOKENS - 1)] - core * OWN) // GROUP
        ready = jnp.where(qb + 1 == hi, OWN // GROUP, ready)
        lax.fori_loop(done, ready, finish, 0)
        return ready

    lax.fori_loop(lo, hi, block, 0)
    for n in range(OWN // GROUP):
        out_copy(n).wait()


def attention(q, k, ssq, table, documents, span_ids):
    vmem = pl.BlockSpec(memory_space=pltpu.VMEM)
    return pl.pallas_call(
        attention_kernel,
        name="attention",
        out_shape=jax.ShapeDtypeStruct((OWN, 2, NS), F32),
        in_specs=[vmem] * 6 + [pl.BlockSpec(memory_space=pltpu.SMEM)],
        out_specs=pl.BlockSpec(memory_space=pl.ANY),
        scratch_shapes=[
            pltpu.VMEM((TOKENS, HD), BF16),
            pltpu.VMEM((TOKENS // KB, WIN, KB), BF16),
            pltpu.VMEM((2 * QB, HD), BF16),
            pltpu.VMEM((6, 2 * QB, KB), F32),
            pltpu.VMEM((2 * QB, 128), F32),
            pltpu.VMEM((2 * QB, 128), F32),
            pltpu.VMEM((2 * QB, NS + 256), F32),
            pltpu.VMEM((2, OWN + 272, NS), F32),
            pltpu.VMEM((OWN + 272, 128), F32),
            pltpu.VMEM((OWN, 2, NS), F32),
            pltpu.SemaphoreType.DMA((8,)),
        ],
        compiler_params=pltpu.CompilerParams(vmem_limit_bytes=32 * 1024 * 1024),
    )(q, k, ssq, table, documents.reshape(16, 128), span_ids.reshape(16, 128), span_ids)


def angle_table():
    i = np.arange(HD // 2, dtype=np.float64)
    f = 500000.0 ** (-i / (HD // 2))
    w = 2.0 * np.pi / f
    s = (8192.0 / w - 1.0) / 3.0
    f = np.where(w < 2048.0, f, np.where(w > 8192.0, f / 8.0, (1.0 - s) * f / 8.0 + s * f))
    phase = np.arange(TOKENS, dtype=np.float64)[:, None] * f[None, :]
    return np.concatenate([np.cos(phase), np.sin(phase)], axis=1).astype(np.float32)


def local(tokens, norm_gain, query_weight, key_weight, documents, span_ids):
    q, k, ssq = project(tokens, norm_gain.reshape(1, -1), query_weight, key_weight)
    table = jnp.asarray(angle_table())
    return attention(
        q.reshape(16, 2 * SUB, HD), k.reshape(TOKENS, HD), ssq, table, documents, span_ids
    )


def solution(mesh):
    finer = Mesh(
        mesh.devices.reshape(mesh.shape["blk"], 4, 4, mesh.shape["kv"]),
        (Y, X, Z, CORE),
    )
    return jax.shard_map(
        local,
        mesh=finer,
        in_specs=(P((Y, CORE), MP), P(MP), P(MP, Y), P(MP, Y), P(), P()),
        out_specs=P(CORE, BLK_MP, None),
        check_vma=False,
    )
```

```python
import functools
import math

import jax
import jax.numpy as jnp
import numpy as np
from jax import lax
from jax.experimental import pallas as pl
from jax.experimental.pallas import tpu as pltpu
from jax.sharding import Mesh
from jax.sharding import PartitionSpec as P

D = 16384
HD = 128
TOKENS = 2048
NS = 1024
X, Z, Y, CORE = "mp_0", "mp_1", "blk", "kv"
MP = (X, Z)
BLK_MP = (Y, X, Z)
MESH = pl.DeviceIdType.MESH
F32 = jnp.float32
BF16 = jnp.bfloat16
RING = 4
CH = 8
R = 128
KI = 5
LAGS = (1, 3, 5, 7)
K_LAGS = (1, 2, 3, 4)
LAST = max(CH - 1 + LAGS[3], KI + K_LAGS[3] + 3)
WS = 8
SLOT_A = {2: 0, 1: 2, 3: 1, 0: 3}
SLOT_B = {2: 1, 1: 0, 3: 2, 0: 3}
ORDER = (2, 1, 3, 0)
PEERS = [(ox, oz) for ox in range(4) for oz in range(4) if (ox, oz) != (0, 0)]


def step(pos, by):
    return lax.rem(pos + by, RING)


def piece_of(i):
    half = lax.rem(i + i // 4 + i // 6, 2)
    far = i // 6
    other = (i + 4) // 6
    offset = other * (1 - far) * (3 - 2 * lax.rem(i, 2)) + 2 * far
    return offset, half


def first_send(st, r, ssem, rsem, axis, d):
    target = step(lax.axis_index(axis), 1 if d == 0 else 3)
    return pltpu.make_async_remote_copy(
        src_ref=st.at[d],
        dst_ref=r.at[d],
        send_sem=ssem.at[0, d],
        recv_sem=rsem.at[0, d],
        device_id={axis: target},
        device_id_type=MESH,
    )


def second_send(st, rb, ssem, rsem, axis, d):
    h = st.shape[1] // 2
    target = step(lax.axis_index(axis), 1 if d == 0 else 3)
    rows = pl.ds(d * h, h)
    return pltpu.make_async_remote_copy(
        src_ref=st.at[2, rows],
        dst_ref=rb.at[rows],
        send_sem=ssem.at[1, d],
        recv_sem=rsem.at[1, d],
        device_id={axis: target},
        device_id_type=MESH,
    )


def add_far(st, r):
    h = st.shape[1] // 2
    st[2, :h] = (st[2, :h].astype(F32) + r[0, :h].astype(F32)).astype(BF16)
    st[2, h:] = (st[2, h:].astype(F32) + r[1, h:].astype(F32)).astype(BF16)


def total_of(st, r, rb, lo, n):
    h = st.shape[1] // 2
    lanes = pl.ds(lo, n)
    top = st[3, :h, lanes].astype(F32) + r[1, :h, lanes].astype(F32) + rb[:h, lanes].astype(F32)
    low = st[3, h:, lanes].astype(F32) + r[0, h:, lanes].astype(F32) + rb[h:, lanes].astype(F32)
    return top.astype(BF16), low.astype(BF16)


def put(st, offset, lo, n, top, low):
    h = st.shape[1] // 2
    st[SLOT_A[offset], :h, lo : lo + n] = top
    st[SLOT_B[offset], h:, lo : lo + n] = low


def project_kernel(
    tok_hbm, gain_ref, w_hbm, kw_hbm, q_out, k_out, ssq_out,
    tok, xs, wbuf, kwbuf, st1, r1, r1b, st2, r2, r2b,
    kpart, kst1, kr1, kr1b, kst2, kr2, kr2b, kfin,
    ssq_own, ssq_in, ssq_sum, ssq_far,
    load_sem, w_sem, g_send, g_recv, s_send, s_recv, k_send, k_recv,
    a_send, a_recv, n_send, n_recv, d_send, d_recv, e_send, e_recv,
):
    x, z, y, core = (lax.axis_index(a) for a in (X, Z, Y, CORE))
    axes = (X, Z)
    barrier = pltpu.get_barrier_semaphore()
    for axis, pos in ((X, x), (Z, z), (Y, y)):
        for by in (1, 3):
            pl.semaphore_signal(barrier, 1, device_id={axis: step(pos, by)}, device_id_type=MESH)
    pl.semaphore_signal(barrier, 1, device_id={CORE: 1 - core}, device_id_type=MESH)

    def tok_load(p):
        return pltpu.make_async_copy(tok_hbm.at[pl.ds(p * R, R)], tok.at[p], load_sem.at[p])

    slab = w_hbm.shape[0] // WS

    def w_load(n):
        rows = pl.ds(n * slab, slab)
        return pltpu.make_async_copy(w_hbm.at[rows], wbuf.at[rows], w_sem.at[n])

    kw_load = pltpu.make_async_copy(kw_hbm, kwbuf, load_sem.at[2])
    for p in range(2):
        tok_load(p).start()
    for n in range(WS):
        w_load(n).start()
    kw_load.start()

    gain = gain_ref[...].astype(F32).reshape(1, -1)

    def scale(p):
        xs[p * R : (p + 1) * R] = (tok[p].astype(F32) * gain).astype(BF16)

    def gather(n, src, dst, by):
        return pltpu.make_async_remote_copy(
            src_ref=tok.at[src],
            dst_ref=tok.at[dst],
            send_sem=g_send.at[n],
            recv_sem=g_recv.at[n],
            device_id={Y: step(y, by)},
            device_id_type=MESH,
        )

    gathers = [
        gather(0, 0, 2, 1), gather(1, 1, 3, 3), gather(2, 1, 4, 1),
        gather(3, 0, 5, 3), gather(4, 2, 6, 1), gather(5, 3, 7, 3),
    ]
    for p in range(2):
        tok_load(p).wait()
    pl.semaphore_wait(barrier, 7)
    for n in range(4):
        gathers[n].start()
    for p in range(2):
        scale(p)

    def q_first(c, color, stage, d):
        st, r = (st1, r1) if stage == 0 else (st2, r2)
        axis = axes[color] if stage == 0 else axes[1 - color]
        return first_send(
            st.at[color, c], r.at[color, c], s_send.at[c, color, stage], s_recv.at[c, color, stage], axis, d
        )

    def q_second(c, color, stage, d):
        st, rb = (st1, r1b) if stage == 0 else (st2, r2b)
        axis = axes[color] if stage == 0 else axes[1 - color]
        return second_send(
            st.at[color, c], rb.at[color, c], s_send.at[c, color, stage], s_recv.at[c, color, stage], axis, d
        )

    def k_first(color, stage, d):
        st, r = (kst1, kr1) if stage == 0 else (kst2, kr2)
        axis = axes[color] if stage == 0 else axes[1 - color]
        return first_send(st.at[color], r.at[color], k_send.at[color, stage], k_recv.at[color, stage], axis, d)

    def k_second(color, stage, d):
        st, rb = (kst1, kr1b) if stage == 0 else (kst2, kr2b)
        axis = axes[color] if stage == 0 else axes[1 - color]
        return second_send(st.at[color], rb.at[color], k_send.at[color, stage], k_recv.at[color, stage], axis, d)

    mine = x * 4 + z
    k_off, k_half = piece_of(mine // 2)
    k_blk = step(y, k_off)
    k_slot = k_half * 2 + lax.rem(mine, 2)

    def key_send(n):
        ox, oz = PEERS[n]
        return pltpu.make_async_remote_copy(
            src_ref=kfin.at[step(x, ox) // 2],
            dst_ref=k_out.at[k_blk, core, k_slot],
            send_sem=a_send.at[n],
            recv_sem=a_recv.at[n],
            device_id={X: step(x, ox), Z: step(z, oz)},
            device_id_type=MESH,
        )

    def square_send(n):
        ox, oz = PEERS[n]
        return pltpu.make_async_remote_copy(
            src_ref=ssq_own,
            dst_ref=ssq_in.at[n],
            send_sem=n_send.at[n],
            recv_sem=n_recv.at[n],
            device_id={X: step(x, ox), Z: step(z, oz)},
            device_id_type=MESH,
        )

    def q_share(c):
        off, half = piece_of(c)
        part = q_out.at[step(y, off), core, half]
        return pltpu.make_async_remote_copy(
            src_ref=part,
            dst_ref=part,
            send_sem=d_send.at[c],
            recv_sem=d_recv.at[c],
            device_id={CORE: 1 - core},
            device_id_type=MESH,
        )

    k_share = pltpu.make_async_remote_copy(
        src_ref=k_out.at[:, core],
        dst_ref=k_out.at[:, core],
        send_sem=e_send.at[0],
        recv_sem=e_recv.at[0],
        device_id={CORE: 1 - core},
        device_id_type=MESH,
    )
    square_share = pltpu.make_async_remote_copy(
        src_ref=ssq_sum,
        dst_ref=ssq_far,
        send_sem=e_send.at[1],
        recv_sem=e_recv.at[1],
        device_id={CORE: 1 - core},
        device_id_type=MESH,
    )

    def put_squares(src, whose):
        for c in range(CH):
            off, half = piece_of(jnp.int32(c))
            row = step(y, off) * 4 + whose * 2 + half
            ssq_out[pl.ds(row, 1), :] = src[c : c + 1, :]

    both = [(color, d) for color in range(2) for d in range(2)]

    def start_pair(c):
        lhs = xs[pl.ds(pl.multiple_of(c * R, 2 * R), 2 * R), :]
        for n, ox in enumerate(ORDER):
            for oz in ORDER:
                col = pl.multiple_of((step(x, ox) * 4 + step(z, oz)) * 256, 256)
                out = jnp.dot(lhs, wbuf[:, pl.ds(col, 256)], preferred_element_type=F32).astype(BF16)
                for u in range(2):
                    a, b, e = u * R, u * R + R // 2, u * R + R
                    put(st1.at[0, c + u], ox, oz * HD, HD, out[a:b, :HD], out[b:e, :HD])
                    put(st1.at[1, c + u], oz, ox * HD, HD, out[a:b, HD:], out[b:e, HD:])
            if n == 1:
                q_first(c, 0, 0, 0).start()
            if n == 2:
                q_first(c, 0, 0, 1).start()
        for d in range(2):
            q_first(c, 1, 0, d).start()
        for color, d in both:
            q_first(c + 1, color, 0, d).start()

    eye = lax.broadcasted_iota(jnp.int32, (R, R), 0) == lax.broadcasted_iota(jnp.int32, (R, R), 1)

    def key_part(p, carry):
        kpart[pl.ds(pl.multiple_of(p * R, R), R), :] = jnp.dot(
            xs[pl.ds(pl.multiple_of(p * R, R), R), :], kwbuf[...], preferred_element_type=F32
        ).astype(BF16)
        acc = jnp.zeros((R, 128), F32)
        for j in range(8):
            t = tok[p, :, j * 128 : (j + 1) * 128].astype(F32)
            acc = acc + t * t
        col = jnp.sum(acc, axis=1, keepdims=True)
        ssq_own[pl.ds(p, 1), :] = jnp.sum(jnp.where(eye, col, 0.0), axis=0, keepdims=True)
        return carry

    def key_start():
        for ox in range(4):
            for oz in range(4):
                row = (step(x, ox) * 4 + step(z, oz)) * 64
                rows = kpart[pl.ds(pl.multiple_of(row, 64), 64), :]
                put(kst1.at[0], ox, oz * HD, HD, rows[:32, :HD], rows[32:, :HD])
                put(kst1.at[1], oz, ox * HD, HD, rows[:32, HD:], rows[32:, HD:])
        for color, d in both:
            k_first(color, 0, d).start()

    def q_far(c, stage):
        st, r = (st1, r1) if stage == 0 else (st2, r2)
        for color in range(2):
            for d in range(2):
                q_first(c, color, stage, d).wait_recv()
            add_far(st.at[color, c], r.at[color, c])
            for d in range(2):
                q_second(c, color, stage, d).start()

    def q_turn(c):
        for color in range(2):
            for d in range(2):
                q_second(c, color, 0, d).wait_recv()
            for o in range(4):
                top, low = total_of(st1.at[color, c], r1.at[color, c], r1b.at[color, c], o * HD, HD)
                put(st2.at[color, c], o, 0, HD, top, low)
            for d in range(2):
                q_first(c, color, 1, d).start()

    def q_last(c):
        off, half = piece_of(c)
        blk = step(y, off)
        for color in range(2):
            for d in range(2):
                q_second(c, color, 1, d).wait_recv()
            top, low = total_of(st2.at[color, c], r2.at[color, c], r2b.at[color, c], 0, HD)
            q_out[blk, core, half, color, : R // 2] = top
            q_out[blk, core, half, color, R // 2 :] = low
        q_share(c).start()

    def k_far(stage):
        st, r = (kst1, kr1) if stage == 0 else (kst2, kr2)
        for color in range(2):
            for d in range(2):
                k_first(color, stage, d).wait_recv()
            add_far(st.at[color], r.at[color])
            for d in range(2):
                k_second(color, stage, d).start()

    def k_turn():
        for color in range(2):
            for d in range(2):
                k_second(color, 0, d).wait_recv()
            for o in range(4):
                top, low = total_of(kst1.at[color], kr1.at[color], kr1b.at[color], o * HD, HD)
                put(kst2.at[color], o, 0, HD, top, low)
            for d in range(2):
                k_first(color, 1, d).start()

    def k_last():
        for color in range(2):
            for d in range(2):
                k_second(color, 1, d).wait_recv()
            top, low = total_of(kst2.at[color], kr2.at[color], kr2b.at[color], 0, HD)
            kfin[color, :32] = top
            kfin[color, 32:] = low
        for n in range(len(PEERS)):
            key_send(n).start()
            square_send(n).start()
        k_out[k_blk, core, k_slot] = kfin[x // 2]

    def k_spread():
        total = ssq_own[...]
        for n in range(len(PEERS)):
            square_send(n).wait_recv()
            total = total + ssq_in[n]
        ssq_sum[...] = total
        square_share.start()
        put_squares(ssq_sum, core)
        for n in range(len(PEERS)):
            key_send(n).wait_recv()
        k_share.start()

    q_steps = (lambda c: q_far(c, 0), q_turn, lambda c: q_far(c, 1), q_last)
    k_steps = (lambda: k_far(0), k_turn, lambda: k_far(1), k_last)

    def body(i, carry):
        for lag, k_lag, q_step, k_step in zip(LAGS, K_LAGS, q_steps, k_steps):
            @pl.when((i >= lag) & (i < CH - 1 + lag))
            def _(lag=lag, q_step=q_step):
                q_step(i - lag)

            @pl.when(i == CH - 2 + lag)
            def _(q_step=q_step):
                q_step(CH - 1)

            @pl.when(i == KI + k_lag)
            def _(k_step=k_step):
                k_step()

        @pl.when(i == KI + K_LAGS[3] + 2)
        def _():
            k_spread()

        @pl.when(i == 0)
        def _():
            for n in range(WS):
                w_load(n).wait()

        @pl.when(i == 1)
        def _():
            for n in range(2):
                gathers[n].wait_recv()
                gathers[4 + n].start()
            for p in (2, 3):
                scale(p)

        @pl.when(i == 3)
        def _():
            for n in range(2, 4):
                gathers[n].wait_recv()
            for p in range(4, 6):
                scale(p)

        @pl.when(i == KI)
        def _():
            for n in range(4, 6):
                gathers[n].wait_recv()
            for p in range(6, 8):
                scale(p)

        @pl.when((i < CH - 2) & ((i == 0) | (lax.rem(i, 2) == 1)))
        def _():
            start_pair(i + jnp.minimum(i, 1))

        @pl.when(i == 1)
        def _():
            kw_load.wait()
            lax.fori_loop(0, 4, key_part, 0)

        @pl.when(i == KI)
        def _():
            lax.fori_loop(4, CH, key_part, 0)
            key_start()

        return carry

    lax.fori_loop(0, LAST, body, 0)
    k_share.wait_recv()
    square_share.wait_recv()
    put_squares(ssq_far, 1 - core)

    def drain(c, carry):
        for color, d in both:
            for stage in range(2):
                q_first(c, color, stage, d).wait_send()
                q_second(c, color, stage, d).wait_send()
        q_share(c).wait()
        return carry

    for color, d in both:
        for stage in range(2):
            k_first(color, stage, d).wait_send()
            k_second(color, stage, d).wait_send()
    for copy in gathers:
        copy.wait_send()
    for n in range(len(PEERS)):
        key_send(n).wait_send()
        square_send(n).wait_send()
    k_share.wait_send()
    square_share.wait_send()
    lax.fori_loop(0, CH, drain, 0)


def project(tokens, gain, query_weight, key_weight):
    dma = pltpu.SemaphoreType.DMA
    vmem = pl.BlockSpec(memory_space=pltpu.VMEM)
    hbm = pl.BlockSpec(memory_space=pltpu.HBM)
    n = len(PEERS)
    k = tokens.shape[1]
    return pl.pallas_call(
        project_kernel,
        name="project",
        out_shape=(
            jax.ShapeDtypeStruct((4, 2, 2, 2, R, HD), BF16),
            jax.ShapeDtypeStruct((4, 2, 4, 64, HD), BF16),
            jax.ShapeDtypeStruct((16, 128), F32),
        ),
        in_specs=[hbm, vmem, hbm, hbm],
        out_specs=(vmem, vmem, vmem),
        scratch_shapes=[
            pltpu.VMEM((CH, R, k), BF16),
            pltpu.VMEM((CH * R, k), BF16),
            pltpu.VMEM((k, query_weight.shape[1]), BF16),
            pltpu.VMEM((k, 256), BF16),
            pltpu.VMEM((2, CH, 4, R, 512), BF16),
            pltpu.VMEM((2, CH, 2, R, 512), BF16),
            pltpu.VMEM((2, CH, R, 512), BF16),
            pltpu.VMEM((2, CH, 4, R, HD), BF16),
            pltpu.VMEM((2, CH, 2, R, HD), BF16),
            pltpu.VMEM((2, CH, R, HD), BF16),
            pltpu.VMEM((CH * R, 256), BF16),
            pltpu.VMEM((2, 4, 64, 512), BF16),
            pltpu.VMEM((2, 2, 64, 512), BF16),
            pltpu.VMEM((2, 64, 512), BF16),
            pltpu.VMEM((2, 4, 64, HD), BF16),
            pltpu.VMEM((2, 2, 64, HD), BF16),
            pltpu.VMEM((2, 64, HD), BF16),
            pltpu.VMEM((2, 64, HD), BF16),
            pltpu.VMEM((CH, 128), F32),
            pltpu.VMEM((n, CH, 128), F32),
            pltpu.VMEM((CH, 128), F32),
            pltpu.VMEM((CH, 128), F32),
            dma((3,)), dma((WS,)), dma((6,)), dma((6,)),
            dma((CH, 2, 2, 2, 2)), dma((CH, 2, 2, 2, 2)),
            dma((2, 2, 2, 2)), dma((2, 2, 2, 2)),
            dma((n,)), dma((n,)), dma((n,)), dma((n,)),
            dma((CH,)), dma((CH,)), dma((2,)), dma((2,)),
        ],
        compiler_params=pltpu.CompilerParams(
            collective_id=0, has_side_effects=True, vmem_limit_bytes=56 * 1024 * 1024
        ),
    )(tokens, gain, query_weight, key_weight)


SUB = 128
QB = 256
KB = 256
WIN = 384
PARTS = ((0, 144), (144, 128))
OWN = NS // 2
GROUP = 64
SCALE = math.log2(math.e) / math.sqrt(HD)
NT = (((1,), (1,)), ((), ()))


def attention_kernel(
    q_hbm, k_hbm, ssq_hbm, tab_ref, doc_ref, span_ref, span_smem, out_hbm,
    q_ref, k_ref, ssq_ref, keys, marks, qs, sbuf, peaks, sums, km, tot, cnt, obuf, sem, in_sem,
):
    core = lax.axis_index(CORE)
    loads = [
        pltpu.make_async_copy(src, dst, in_sem.at[n])
        for n, (src, dst) in enumerate(((ssq_hbm, ssq_ref), (k_hbm, k_ref), (q_hbm, q_ref)))
    ]
    for load in loads:
        load.start()
    docs = doc_ref[...]
    spans = span_ref[...]

    def below(a, v):
        return jnp.sum(jnp.where(a < v, 1.0, 0.0)).astype(jnp.int32)

    c1, c2, c3 = below(docs, 1), below(docs, 2), below(docs, 3)
    mid = below(spans, OWN)
    lo = core * mid // QB
    hi = jnp.where(core == 0, (mid + QB - 1) // QB, TOKENS // QB)
    eye = lax.broadcasted_iota(jnp.int32, (SUB, SUB), 0) == lax.broadcasted_iota(jnp.int32, (SUB, SUB), 1)
    low_lanes = lax.broadcasted_iota(jnp.int32, (SUB, HD), 1) < HD // 2

    def start_of(i):
        return jnp.where(i >= c3, c3, jnp.where(i >= c2, c2, jnp.where(i >= c1, c1, 0)))

    turned_fine = pltpu.roll(tab_ref[:SUB, :], HD // 2, 1)

    def tables(b):
        t = tab_ref[pl.ds(SUB + b, 1), :] * tab_ref[:SUB, :] + tab_ref[pl.ds(SUB + 16 + b, 1), :] * turned_fine
        turned = pltpu.roll(t, HD // 2, 1)
        row = lax.rsqrt(ssq_ref[pl.ds(b, 1), :] / D + 1e-05)
        col = jnp.sum(jnp.where(eye, row, 0.0), axis=1, keepdims=True)
        return jnp.where(low_lanes, t, turned) * col, jnp.where(low_lanes, -turned, t) * col

    def turn(v, cosine, sine):
        return v * cosine + pltpu.roll(v, HD // 2, 1) * sine

    def base_of(kb):
        return span_smem[kb * KB] // 128 * 128

    def prepare(kb, carry):
        ids = lax.broadcasted_iota(jnp.int32, (WIN, 128), 0) + base_of(kb)
        for half in range(2):
            b = kb * 2 + half
            cosine, sine = tables(b)
            rows = pl.ds(pl.multiple_of(b * SUB, SUB), SUB)
            keys[rows, :] = turn(k_ref[rows, :].astype(F32), cosine, sine).astype(BF16)
            row = span_ref[pl.ds(b, 1), :]
            marks[kb, :, half * 128 : (half + 1) * 128] = jnp.where(ids == row, 1.0, 0.0).astype(BF16)
        return carry

    tot[...] = jnp.zeros_like(tot)
    cnt[...] = jnp.zeros_like(cnt)
    loads[0].wait()
    loads[1].wait()
    lax.fori_loop(start_of(lo * QB) // KB, hi, prepare, 0)
    loads[2].wait()
    ones = jnp.ones((QB, 128), BF16)

    def out_copy(n):
        rows = pl.ds(pl.multiple_of(n * GROUP, GROUP), GROUP)
        return pltpu.make_async_copy(obuf.at[rows], out_hbm.at[rows], sem.at[n])

    def finish(n, carry):
        rows = pl.ds(pl.multiple_of(n * GROUP, GROUP), GROUP)
        share = 1.0 / cnt[rows, :]
        for h in range(2):
            for j in range(NS // 128):
                lanes = slice(j * 128, (j + 1) * 128)
                obuf[rows, h, lanes] = jnp.log(tot[h, rows, lanes] * share + 1e-06)
        out_copy(n).start()
        return carry

    def block(qb, done):
        first = qb * QB
        for u in range(2):
            cosine, sine = tables(qb * 2 + u)
            for h in range(2):
                v = q_ref[qb * 2 + u, h * SUB : (h + 1) * SUB, :].astype(F32)
                at = h * QB + u * SUB
                qs[at : at + SUB, :] = (turn(v, cosine, sine) * SCALE).astype(BF16)
        kb0 = start_of(first) // KB
        last = span_smem[first + QB - 1]
        tile0 = base_of(kb0) // 256

        peaks[...] = jnp.full_like(peaks, -1e30)

        def score(kb, carry):
            block_keys = keys[pl.ds(pl.multiple_of(kb * KB, KB), KB), :]
            s = lax.dot_general(qs[...], block_keys, NT, preferred_element_type=F32)
            cols = lax.broadcasted_iota(jnp.int32, (SUB, KB), 1) + kb * KB
            for u in range(2):
                rows = lax.broadcasted_iota(jnp.int32, (SUB, 1), 0) + (first + u * SUB)
                seen = (cols <= rows) & (cols >= start_of(rows))
                for h in range(2):
                    at = slice(h * QB + u * SUB, h * QB + (u + 1) * SUB)
                    part = jnp.where(seen, s[at], -1e30)
                    sbuf[kb - kb0, at, :] = part
                    peaks[at, :] = jnp.maximum(peaks[at, :], jnp.maximum(part[:, :128], part[:, 128:]))
            return carry

        lax.fori_loop(kb0, qb + 1, score, 0)
        peak = jnp.max(peaks[...], axis=1, keepdims=True)
        sums[...] = jnp.zeros_like(sums)

        def clear(t, carry):
            km[:, pl.ds(pl.multiple_of(t * 256, 256), 256)] = jnp.zeros((2 * QB, 256), F32)
            return carry

        lax.fori_loop(tile0, jnp.maximum(base_of(qb) + WIN - 1, last) // 256 + 1, clear, 0)

        def mass(kb, carry):
            e = jnp.exp2(sbuf[kb - kb0] - peak)
            sums[...] = sums[...] + e[:, :128] + e[:, 128:]
            got = lax.dot_general(e.astype(BF16), marks[kb], NT, preferred_element_type=F32)
            lanes = pl.ds(pl.multiple_of(base_of(kb), 128), WIN)
            km[:, lanes] = km[:, lanes] + got
            return carry

        lax.fori_loop(kb0, qb + 1, mass, 0)
        scale = 1.0 / jnp.sum(sums[...], axis=1, keepdims=True)
        lead = jnp.maximum(span_smem[first] - core * OWN, 0) // 8 * 8
        row = jnp.concatenate([span_ref[pl.ds(qb * 2, 1), :], span_ref[pl.ds(qb * 2 + 1, 1), :]], axis=1)

        def gather_part(lo_row, n):
            ids = lax.broadcasted_iota(jnp.int32, (n, QB), 0) + (lead + lo_row + core * OWN)
            pick = jnp.where(ids == row, 1.0, 0.0).astype(BF16)
            at = pl.ds(pl.multiple_of(lead + lo_row, 8), n)

            def tile(t, carry):
                lanes = pl.ds(pl.multiple_of(t * 256, 256), 256)
                for h in range(2):
                    hs = slice(h * QB, (h + 1) * QB)
                    part = (km[hs, lanes] * scale[hs]).astype(BF16)
                    tot[h, at, lanes] = tot[h, at, lanes] + jnp.dot(pick, part, preferred_element_type=F32)
                return carry

            lax.fori_loop(tile0, last // 256 + 1, tile, 0)
            cnt[at, :] = cnt[at, :] + jnp.dot(pick, ones, preferred_element_type=F32)

        gather_part(*PARTS[0])

        @pl.when(last - core * OWN >= lead + PARTS[1][0])
        def _():
            gather_part(*PARTS[1])

        ready = (span_smem[jnp.minimum(first + QB, TOKENS - 1)] - core * OWN) // GROUP
        ready = jnp.where(qb + 1 == hi, OWN // GROUP, ready)
        lax.fori_loop(done, ready, finish, 0)
        return ready

    lax.fori_loop(lo, hi, block, 0)
    for n in range(OWN // GROUP):
        out_copy(n).wait()


def attention(q, k, ssq, table, documents, span_ids):
    vmem = pl.BlockSpec(memory_space=pltpu.VMEM)
    return pl.pallas_call(
        attention_kernel,
        name="attention",
        out_shape=jax.ShapeDtypeStruct((OWN, 2, NS), F32),
        in_specs=[pl.BlockSpec(memory_space=pl.ANY)] * 3 + [vmem] * 3 + [pl.BlockSpec(memory_space=pltpu.SMEM)],
        out_specs=pl.BlockSpec(memory_space=pl.ANY),
        scratch_shapes=[
            pltpu.VMEM(q.shape, BF16),
            pltpu.VMEM(k.shape, BF16),
            pltpu.VMEM(ssq.shape, F32),
            pltpu.VMEM((TOKENS, HD), BF16),
            pltpu.VMEM((TOKENS // KB, WIN, KB), BF16),
            pltpu.VMEM((2 * QB, HD), BF16),
            pltpu.VMEM((6, 2 * QB, KB), F32),
            pltpu.VMEM((2 * QB, 128), F32),
            pltpu.VMEM((2 * QB, 128), F32),
            pltpu.VMEM((2 * QB, NS + 256), F32),
            pltpu.VMEM((2, OWN + 272, NS), F32),
            pltpu.VMEM((OWN + 272, 128), F32),
            pltpu.VMEM((OWN, 2, NS), F32),
            pltpu.SemaphoreType.DMA((8,)),
            pltpu.SemaphoreType.DMA((3,)),
        ],
        compiler_params=pltpu.CompilerParams(vmem_limit_bytes=60 * 1024 * 1024),
    )(q, k, ssq, table, documents.reshape(16, 128), span_ids.reshape(16, 128), span_ids)


def angle_table():
    i = np.arange(HD // 2, dtype=np.float64)
    f = 500000.0 ** (-i / (HD // 2))
    w = 2.0 * np.pi / f
    s = (8192.0 / w - 1.0) / 3.0
    f = np.where(w < 2048.0, f, np.where(w > 8192.0, f / 8.0, (1.0 - s) * f / 8.0 + s * f))
    fine = np.arange(SUB, dtype=np.float64)[:, None] * f[None, :]
    coarse = np.arange(0, TOKENS, SUB, dtype=np.float64)[:, None] * f[None, :]
    rows = [
        np.concatenate([np.cos(fine), np.sin(fine)], axis=1),
        np.concatenate([np.cos(coarse), np.cos(coarse)], axis=1),
        np.concatenate([-np.sin(coarse), np.sin(coarse)], axis=1),
    ]
    return np.concatenate(rows, axis=0).astype(np.float32)


def local(tokens, norm_gain, query_weight, key_weight, documents, span_ids):
    q, k, ssq = project(tokens, norm_gain, query_weight, key_weight)
    table = jnp.asarray(angle_table())
    return attention(
        q.reshape(16, 2 * SUB, HD), k.reshape(TOKENS, HD), ssq, table, documents, span_ids
    )


def solution(mesh):
    finer = Mesh(
        mesh.devices.reshape(mesh.shape["blk"], 4, 4, mesh.shape["kv"]),
        (Y, X, Z, CORE),
    )
    return jax.shard_map(
        local,
        mesh=finer,
        in_specs=(P((Y, CORE), MP), P(MP), P(MP, Y), P(MP, Y), P(), P()),
        out_specs=P(CORE, BLK_MP, None),
        check_vma=False,
    )
```

```python
import functools
import math

import jax
import jax.numpy as jnp
import numpy as np
from jax import lax
from jax.experimental import pallas as pl
from jax.experimental.pallas import tpu as pltpu
from jax.sharding import Mesh
from jax.sharding import PartitionSpec as P

D = 16384
HD = 128
TOKENS = 2048
NS = 1024
X, Z, Y, CORE = "mp_0", "mp_1", "blk", "kv"
MP = (X, Z)
BLK_MP = (Y, X, Z)
MESH = pl.DeviceIdType.MESH
F32 = jnp.float32
BF16 = jnp.bfloat16
RING = 4
CH = 8
R = 128
KI = 5
LAGS = (1, 3, 5, 7)
K_LAGS = (1, 2, 3, 4)
LAST = max(CH - 2, KI + 1) + max(LAGS[3], K_LAGS[3] + 2) + 1
WS = 8
SLOT_A = {2: 0, 1: 2, 3: 1, 0: 3}
SLOT_B = {2: 1, 1: 0, 3: 2, 0: 3}
ORDER = (2, 1, 3, 0)
PEERS = [(ox, oz) for ox in range(4) for oz in range(4) if (ox, oz) != (0, 0)]


def step(pos, by):
    return lax.rem(pos + by, RING)


def piece_of(i):
    half = lax.rem(i + i // 4 + i // 6, 2)
    far = i // 6
    other = (i + 4) // 6
    offset = other * (1 - far) * (3 - 2 * lax.rem(i, 2)) + 2 * far
    return offset, half


def first_send(st, r, ssem, rsem, axis, d):
    target = step(lax.axis_index(axis), 1 if d == 0 else 3)
    return pltpu.make_async_remote_copy(
        src_ref=st.at[d],
        dst_ref=r.at[d],
        send_sem=ssem.at[0, d],
        recv_sem=rsem.at[0, d],
        device_id={axis: target},
        device_id_type=MESH,
    )


def second_send(st, rb, ssem, rsem, axis, d):
    h = st.shape[1] // 2
    target = step(lax.axis_index(axis), 1 if d == 0 else 3)
    rows = pl.ds(d * h, h)
    return pltpu.make_async_remote_copy(
        src_ref=st.at[2, rows],
        dst_ref=rb.at[rows],
        send_sem=ssem.at[1, d],
        recv_sem=rsem.at[1, d],
        device_id={axis: target},
        device_id_type=MESH,
    )


def add_far(st, r):
    h = st.shape[1] // 2
    st[2, :h] = (st[2, :h].astype(F32) + r[0, :h].astype(F32)).astype(BF16)
    st[2, h:] = (st[2, h:].astype(F32) + r[1, h:].astype(F32)).astype(BF16)


def total_of(st, r, rb, lo, n):
    h = st.shape[1] // 2
    lanes = pl.ds(lo, n)
    top = st[3, :h, lanes].astype(F32) + r[1, :h, lanes].astype(F32) + rb[:h, lanes].astype(F32)
    low = st[3, h:, lanes].astype(F32) + r[0, h:, lanes].astype(F32) + rb[h:, lanes].astype(F32)
    return top.astype(BF16), low.astype(BF16)


def put(st, offset, lo, n, top, low):
    h = st.shape[1] // 2
    st[SLOT_A[offset], :h, lo : lo + n] = top
    st[SLOT_B[offset], h:, lo : lo + n] = low


def project_kernel(
    tok_hbm, gain_ref, w_hbm, kw_hbm, q_out, k_out, ssq_out,
    tok, xs, wbuf, kwbuf, st1, r1, r1b, st2, r2, r2b,
    kpart, kst1, kr1, kr1b, kst2, kr2, kr2b, kfin,
    ssq_own, ssq_in, ssq_sum, ssq_far,
    load_sem, w_sem, g_send, g_recv, s_send, s_recv, k_send, k_recv,
    a_send, a_recv, n_send, n_recv, d_send, d_recv, e_send, e_recv,
):
    x, z, y, core = (lax.axis_index(a) for a in (X, Z, Y, CORE))
    axes = (X, Z)
    barrier = pltpu.get_barrier_semaphore()
    for axis, pos in ((X, x), (Z, z), (Y, y)):
        for by in (1, 3):
            pl.semaphore_signal(barrier, 1, device_id={axis: step(pos, by)}, device_id_type=MESH)
    pl.semaphore_signal(barrier, 1, device_id={CORE: 1 - core}, device_id_type=MESH)

    def tok_load(p):
        return pltpu.make_async_copy(tok_hbm.at[pl.ds(p * R, R)], tok.at[p], load_sem.at[p])

    slab = w_hbm.shape[0] // WS

    def w_load(n):
        rows = pl.ds(n * slab, slab)
        return pltpu.make_async_copy(w_hbm.at[rows], wbuf.at[rows], w_sem.at[n])

    kw_load = pltpu.make_async_copy(kw_hbm, kwbuf, load_sem.at[2])
    for p in range(2):
        tok_load(p).start()
    for n in range(WS):
        w_load(n).start()
    kw_load.start()

    gain = gain_ref[...].astype(F32).reshape(1, -1)

    def scale(p):
        xs[p * R : (p + 1) * R] = (tok[p].astype(F32) * gain).astype(BF16)

    def gather(n, src, dst, by):
        return pltpu.make_async_remote_copy(
            src_ref=tok.at[src],
            dst_ref=tok.at[dst],
            send_sem=g_send.at[n],
            recv_sem=g_recv.at[n],
            device_id={Y: step(y, by)},
            device_id_type=MESH,
        )

    gathers = [
        gather(0, 0, 2, 1), gather(1, 1, 3, 3), gather(2, 1, 4, 1),
        gather(3, 0, 5, 3), gather(4, 2, 6, 1), gather(5, 3, 7, 3),
    ]
    for p in range(2):
        tok_load(p).wait()
    pl.semaphore_wait(barrier, 7)
    for n in range(4):
        gathers[n].start()
    for p in range(2):
        scale(p)

    def q_first(c, color, stage, d):
        st, r = (st1, r1) if stage == 0 else (st2, r2)
        axis = axes[color] if stage == 0 else axes[1 - color]
        return first_send(
            st.at[color, c], r.at[color, c], s_send.at[c, color, stage], s_recv.at[c, color, stage], axis, d
        )

    def q_second(c, color, stage, d):
        st, rb = (st1, r1b) if stage == 0 else (st2, r2b)
        axis = axes[color] if stage == 0 else axes[1 - color]
        return second_send(
            st.at[color, c], rb.at[color, c], s_send.at[c, color, stage], s_recv.at[c, color, stage], axis, d
        )

    def k_first(color, stage, d):
        st, r = (kst1, kr1) if stage == 0 else (kst2, kr2)
        axis = axes[color] if stage == 0 else axes[1 - color]
        return first_send(st.at[color], r.at[color], k_send.at[color, stage], k_recv.at[color, stage], axis, d)

    def k_second(color, stage, d):
        st, rb = (kst1, kr1b) if stage == 0 else (kst2, kr2b)
        axis = axes[color] if stage == 0 else axes[1 - color]
        return second_send(st.at[color], rb.at[color], k_send.at[color, stage], k_recv.at[color, stage], axis, d)

    mine = x * 4 + z
    k_off, k_half = piece_of(mine // 2)
    k_blk = step(y, k_off)
    k_slot = k_half * 2 + lax.rem(mine, 2)

    def key_send(n):
        ox, oz = PEERS[n]
        return pltpu.make_async_remote_copy(
            src_ref=kfin.at[step(x, ox) // 2],
            dst_ref=k_out.at[k_blk, core, k_slot],
            send_sem=a_send.at[n],
            recv_sem=a_recv.at[n],
            device_id={X: step(x, ox), Z: step(z, oz)},
            device_id_type=MESH,
        )

    def square_send(n):
        ox, oz = PEERS[n]
        return pltpu.make_async_remote_copy(
            src_ref=ssq_own,
            dst_ref=ssq_in.at[n],
            send_sem=n_send.at[n],
            recv_sem=n_recv.at[n],
            device_id={X: step(x, ox), Z: step(z, oz)},
            device_id_type=MESH,
        )

    def q_share(c):
        off, half = piece_of(c)
        part = q_out.at[step(y, off), core, half]
        return pltpu.make_async_remote_copy(
            src_ref=part,
            dst_ref=part,
            send_sem=d_send.at[c],
            recv_sem=d_recv.at[c],
            device_id={CORE: 1 - core},
            device_id_type=MESH,
        )

    k_share = pltpu.make_async_remote_copy(
        src_ref=k_out.at[:, core],
        dst_ref=k_out.at[:, core],
        send_sem=e_send.at[0],
        recv_sem=e_recv.at[0],
        device_id={CORE: 1 - core},
        device_id_type=MESH,
    )
    square_share = pltpu.make_async_remote_copy(
        src_ref=ssq_sum,
        dst_ref=ssq_far,
        send_sem=e_send.at[1],
        recv_sem=e_recv.at[1],
        device_id={CORE: 1 - core},
        device_id_type=MESH,
    )

    def put_squares(src, whose):
        for c in range(CH):
            off, half = piece_of(jnp.int32(c))
            row = step(y, off) * 4 + whose * 2 + half
            ssq_out[pl.ds(row, 1), :] = src[c : c + 1, :]

    both = [(color, d) for color in range(2) for d in range(2)]

    def start_pair(c):
        lhs = xs[pl.ds(pl.multiple_of(c * R, 2 * R), 2 * R), :]
        for n, ox in enumerate(ORDER):
            for oz in ORDER:
                col = pl.multiple_of((step(x, ox) * 4 + step(z, oz)) * 256, 256)
                out = jnp.dot(lhs, wbuf[:, pl.ds(col, 256)], preferred_element_type=F32).astype(BF16)
                for u in range(2):
                    a, b, e = u * R, u * R + R // 2, u * R + R
                    put(st1.at[0, c + u], ox, oz * HD, HD, out[a:b, :HD], out[b:e, :HD])
                    put(st1.at[1, c + u], oz, ox * HD, HD, out[a:b, HD:], out[b:e, HD:])
            if n == 1:
                q_first(c, 0, 0, 0).start()
            if n == 2:
                q_first(c, 0, 0, 1).start()
        for d in range(2):
            q_first(c, 1, 0, d).start()
        for color, d in both:
            q_first(c + 1, color, 0, d).start()

    eye = lax.broadcasted_iota(jnp.int32, (R, R), 0) == lax.broadcasted_iota(jnp.int32, (R, R), 1)

    def key_part(p, carry):
        kpart[pl.ds(pl.multiple_of(p * R, R), R), :] = jnp.dot(
            xs[pl.ds(pl.multiple_of(p * R, R), R), :], kwbuf[...], preferred_element_type=F32
        ).astype(BF16)
        acc = jnp.zeros((R, 128), F32)
        for j in range(8):
            t = tok[p, :, j * 128 : (j + 1) * 128].astype(F32)
            acc = acc + t * t
        col = jnp.sum(acc, axis=1, keepdims=True)
        ssq_own[pl.ds(p, 1), :] = jnp.sum(jnp.where(eye, col, 0.0), axis=0, keepdims=True)
        return carry

    def key_start():
        for ox in range(4):
            for oz in range(4):
                row = (step(x, ox) * 4 + step(z, oz)) * 64
                rows = kpart[pl.ds(pl.multiple_of(row, 64), 64), :]
                put(kst1.at[0], ox, oz * HD, HD, rows[:32, :HD], rows[32:, :HD])
                put(kst1.at[1], oz, ox * HD, HD, rows[:32, HD:], rows[32:, HD:])
        for color, d in both:
            k_first(color, 0, d).start()

    def q_far(c, stage):
        st, r = (st1, r1) if stage == 0 else (st2, r2)
        for color in range(2):
            for d in range(2):
                q_first(c, color, stage, d).wait_recv()
            add_far(st.at[color, c], r.at[color, c])
            for d in range(2):
                q_second(c, color, stage, d).start()

    def q_turn(c):
        for color in range(2):
            for d in range(2):
                q_second(c, color, 0, d).wait_recv()
            for o in range(4):
                top, low = total_of(st1.at[color, c], r1.at[color, c], r1b.at[color, c], o * HD, HD)
                put(st2.at[color, c], o, 0, HD, top, low)
            for d in range(2):
                q_first(c, color, 1, d).start()

    def q_last(c):
        off, half = piece_of(c)
        blk = step(y, off)
        for color in range(2):
            for d in range(2):
                q_second(c, color, 1, d).wait_recv()
            top, low = total_of(st2.at[color, c], r2.at[color, c], r2b.at[color, c], 0, HD)
            q_out[blk, core, half, color, : R // 2] = top
            q_out[blk, core, half, color, R // 2 :] = low
        q_share(c).start()

    def k_far(stage):
        st, r = (kst1, kr1) if stage == 0 else (kst2, kr2)
        for color in range(2):
            for d in range(2):
                k_first(color, stage, d).wait_recv()
            add_far(st.at[color], r.at[color])
            for d in range(2):
                k_second(color, stage, d).start()

    def k_turn():
        for color in range(2):
            for d in range(2):
                k_second(color, 0, d).wait_recv()
            for o in range(4):
                top, low = total_of(kst1.at[color], kr1.at[color], kr1b.at[color], o * HD, HD)
                put(kst2.at[color], o, 0, HD, top, low)
            for d in range(2):
                k_first(color, 1, d).start()

    def k_last():
        for color in range(2):
            for d in range(2):
                k_second(color, 1, d).wait_recv()
            top, low = total_of(kst2.at[color], kr2.at[color], kr2b.at[color], 0, HD)
            kfin[color, :32] = top
            kfin[color, 32:] = low
        for n in range(len(PEERS)):
            key_send(n).start()
            square_send(n).start()
        k_out[k_blk, core, k_slot] = kfin[x // 2]

    def k_spread():
        total = ssq_own[...]
        for n in range(len(PEERS)):
            square_send(n).wait_recv()
            total = total + ssq_in[n]
        ssq_sum[...] = total
        square_share.start()
        put_squares(ssq_sum, core)
        for n in range(len(PEERS)):
            key_send(n).wait_recv()
        k_share.start()

    q_steps = (lambda c: q_far(c, 0), q_turn, lambda c: q_far(c, 1), q_last)
    k_steps = (lambda: k_far(0), k_turn, lambda: k_far(1), k_last)

    def body(i, carry):
        for lag, k_lag, q_step, k_step in zip(LAGS, K_LAGS, q_steps, k_steps):
            @pl.when((i >= lag) & (i < CH - 2 + lag))
            def _(lag=lag, q_step=q_step):
                q_step(i - lag)

            @pl.when(i == KI + 1 + lag)
            def _(q_step=q_step):
                q_step(CH - 2)
                q_step(CH - 1)

            @pl.when(i == KI + k_lag)
            def _(k_step=k_step):
                k_step()

        @pl.when(i == KI + K_LAGS[3] + 2)
        def _():
            k_spread()

        @pl.when(i == 0)
        def _():
            for n in range(WS):
                w_load(n).wait()

        @pl.when(i == 1)
        def _():
            for n in range(2):
                gathers[n].wait_recv()
                gathers[4 + n].start()
            for p in (2, 3):
                scale(p)

        @pl.when(i == 3)
        def _():
            for n in range(2, 4):
                gathers[n].wait_recv()
            for p in range(4, 6):
                scale(p)

        @pl.when(i == KI)
        def _():
            for n in range(4, 6):
                gathers[n].wait_recv()
            for p in range(6, 8):
                scale(p)

        @pl.when(i == KI)
        def _():
            lax.fori_loop(4, CH, key_part, 0)
            key_start()

        @pl.when((i == 0) | (i == 1) | (i == 3) | (i == KI))
        def _():
            start_pair(jnp.minimum(i + jnp.minimum(i, 1), CH - 2))

        @pl.when(i == 1)
        def _():
            kw_load.wait()
            lax.fori_loop(0, 4, key_part, 0)

        return carry

    lax.fori_loop(0, LAST, body, 0)
    k_share.wait_recv()
    square_share.wait_recv()
    put_squares(ssq_far, 1 - core)

    def drain(c, carry):
        for color, d in both:
            for stage in range(2):
                q_first(c, color, stage, d).wait_send()
                q_second(c, color, stage, d).wait_send()
        q_share(c).wait()
        return carry

    for color, d in both:
        for stage in range(2):
            k_first(color, stage, d).wait_send()
            k_second(color, stage, d).wait_send()
    for copy in gathers:
        copy.wait_send()
    for n in range(len(PEERS)):
        key_send(n).wait_send()
        square_send(n).wait_send()
    k_share.wait_send()
    square_share.wait_send()
    lax.fori_loop(0, CH, drain, 0)


def project(tokens, gain, query_weight, key_weight):
    dma = pltpu.SemaphoreType.DMA
    vmem = pl.BlockSpec(memory_space=pltpu.VMEM)
    hbm = pl.BlockSpec(memory_space=pltpu.HBM)
    n = len(PEERS)
    k = tokens.shape[1]
    return pl.pallas_call(
        project_kernel,
        name="project",
        out_shape=(
            jax.ShapeDtypeStruct((4, 2, 2, 2, R, HD), BF16),
            jax.ShapeDtypeStruct((4, 2, 4, 64, HD), BF16),
            jax.ShapeDtypeStruct((16, 128), F32),
        ),
        in_specs=[hbm, vmem, hbm, hbm],
        out_specs=(vmem, vmem, vmem),
        scratch_shapes=[
            pltpu.VMEM((CH, R, k), BF16),
            pltpu.VMEM((CH * R, k), BF16),
            pltpu.VMEM((k, query_weight.shape[1]), BF16),
            pltpu.VMEM((k, 256), BF16),
            pltpu.VMEM((2, CH, 4, R, 512), BF16),
            pltpu.VMEM((2, CH, 2, R, 512), BF16),
            pltpu.VMEM((2, CH, R, 512), BF16),
            pltpu.VMEM((2, CH, 4, R, HD), BF16),
            pltpu.VMEM((2, CH, 2, R, HD), BF16),
            pltpu.VMEM((2, CH, R, HD), BF16),
            pltpu.VMEM((CH * R, 256), BF16),
            pltpu.VMEM((2, 4, 64, 512), BF16),
            pltpu.VMEM((2, 2, 64, 512), BF16),
            pltpu.VMEM((2, 64, 512), BF16),
            pltpu.VMEM((2, 4, 64, HD), BF16),
            pltpu.VMEM((2, 2, 64, HD), BF16),
            pltpu.VMEM((2, 64, HD), BF16),
            pltpu.VMEM((2, 64, HD), BF16),
            pltpu.VMEM((CH, 128), F32),
            pltpu.VMEM((n, CH, 128), F32),
            pltpu.VMEM((CH, 128), F32),
            pltpu.VMEM((CH, 128), F32),
            dma((3,)), dma((WS,)), dma((6,)), dma((6,)),
            dma((CH, 2, 2, 2, 2)), dma((CH, 2, 2, 2, 2)),
            dma((2, 2, 2, 2)), dma((2, 2, 2, 2)),
            dma((n,)), dma((n,)), dma((n,)), dma((n,)),
            dma((CH,)), dma((CH,)), dma((2,)), dma((2,)),
        ],
        compiler_params=pltpu.CompilerParams(
            collective_id=0, has_side_effects=True, vmem_limit_bytes=56 * 1024 * 1024
        ),
    )(tokens, gain, query_weight, key_weight)


SUB = 128
QB = 256
KB = 256
WIN = 384
PARTS = ((0, 144), (144, 128))
OWN = NS // 2
GROUP = 64
SCALE = math.log2(math.e) / math.sqrt(HD)
NT = (((1,), (1,)), ((), ()))


def attention_kernel(
    q_hbm, k_hbm, ssq_hbm, tab_ref, doc_ref, span_ref, span_smem, out_hbm,
    q_ref, k_ref, ssq_ref, keys, marks, qs, sbuf, peaks, sums, km, tot, cnt, obuf, sem, in_sem,
):
    core = lax.axis_index(CORE)
    loads = [
        pltpu.make_async_copy(src, dst, in_sem.at[n])
        for n, (src, dst) in enumerate(((ssq_hbm, ssq_ref), (k_hbm, k_ref), (q_hbm, q_ref)))
    ]
    for load in loads:
        load.start()
    docs = doc_ref[...]
    spans = span_ref[...]

    def below(a, v):
        return jnp.sum(jnp.where(a < v, 1.0, 0.0)).astype(jnp.int32)

    c1, c2, c3 = below(docs, 1), below(docs, 2), below(docs, 3)
    mid = below(spans, OWN)
    lo = core * mid // QB
    hi = jnp.where(core == 0, (mid + QB - 1) // QB, TOKENS // QB)
    eye = lax.broadcasted_iota(jnp.int32, (SUB, SUB), 0) == lax.broadcasted_iota(jnp.int32, (SUB, SUB), 1)
    low_lanes = lax.broadcasted_iota(jnp.int32, (SUB, HD), 1) < HD // 2

    def start_of(i):
        return jnp.where(i >= c3, c3, jnp.where(i >= c2, c2, jnp.where(i >= c1, c1, 0)))

    turned_fine = pltpu.roll(tab_ref[:SUB, :], HD // 2, 1)

    def tables(b):
        t = tab_ref[pl.ds(SUB + b, 1), :] * tab_ref[:SUB, :] + tab_ref[pl.ds(SUB + 16 + b, 1), :] * turned_fine
        turned = pltpu.roll(t, HD // 2, 1)
        row = lax.rsqrt(ssq_ref[pl.ds(b, 1), :] / D + 1e-05)
        col = jnp.sum(jnp.where(eye, row, 0.0), axis=1, keepdims=True)
        return jnp.where(low_lanes, t, turned) * col, jnp.where(low_lanes, -turned, t) * col

    def turn(v, cosine, sine):
        return v * cosine + pltpu.roll(v, HD // 2, 1) * sine

    def base_of(kb):
        return span_smem[kb * KB] // 128 * 128

    def prepare(kb, carry):
        ids = lax.broadcasted_iota(jnp.int32, (WIN, 128), 0) + base_of(kb)
        for half in range(2):
            b = kb * 2 + half
            cosine, sine = tables(b)
            rows = pl.ds(pl.multiple_of(b * SUB, SUB), SUB)
            keys[rows, :] = turn(k_ref[rows, :].astype(F32), cosine, sine).astype(BF16)
            row = span_ref[pl.ds(b, 1), :]
            marks[kb, :, half * 128 : (half + 1) * 128] = jnp.where(ids == row, 1.0, 0.0).astype(BF16)
        return carry

    tot[...] = jnp.zeros_like(tot)
    cnt[...] = jnp.zeros_like(cnt)
    loads[0].wait()
    loads[1].wait()
    lax.fori_loop(start_of(lo * QB) // KB, hi, prepare, 0)
    loads[2].wait()
    ones = jnp.ones((QB, 128), BF16)

    def out_copy(n):
        rows = pl.ds(pl.multiple_of(n * GROUP, GROUP), GROUP)
        return pltpu.make_async_copy(obuf.at[rows], out_hbm.at[rows], sem.at[n])

    def finish(n, carry):
        rows = pl.ds(pl.multiple_of(n * GROUP, GROUP), GROUP)
        share = 1.0 / cnt[rows, :]
        for h in range(2):
            for j in range(NS // 128):
                lanes = slice(j * 128, (j + 1) * 128)
                obuf[rows, h, lanes] = jnp.log(tot[h, rows, lanes] * share + 1e-06)
        out_copy(n).start()
        return carry

    def block(qb, done):
        first = qb * QB
        for u in range(2):
            cosine, sine = tables(qb * 2 + u)
            for h in range(2):
                v = q_ref[qb * 2 + u, h * SUB : (h + 1) * SUB, :].astype(F32)
                at = h * QB + u * SUB
                qs[at : at + SUB, :] = (turn(v, cosine, sine) * SCALE).astype(BF16)
        kb0 = start_of(first) // KB
        last = span_smem[first + QB - 1]
        tile0 = base_of(kb0) // 256

        peaks[...] = jnp.full_like(peaks, -1e30)

        def score(kb, carry):
            block_keys = keys[pl.ds(pl.multiple_of(kb * KB, KB), KB), :]
            s = lax.dot_general(qs[...], block_keys, NT, preferred_element_type=F32)
            cols = lax.broadcasted_iota(jnp.int32, (SUB, KB), 1) + kb * KB
            for u in range(2):
                rows = lax.broadcasted_iota(jnp.int32, (SUB, 1), 0) + (first + u * SUB)
                seen = (cols <= rows) & (cols >= start_of(rows))
                for h in range(2):
                    at = slice(h * QB + u * SUB, h * QB + (u + 1) * SUB)
                    part = jnp.where(seen, s[at], -1e30)
                    sbuf[kb - kb0, at, :] = part
                    peaks[at, :] = jnp.maximum(peaks[at, :], jnp.maximum(part[:, :128], part[:, 128:]))
            return carry

        lax.fori_loop(kb0, qb + 1, score, 0)
        peak = jnp.max(peaks[...], axis=1, keepdims=True)
        sums[...] = jnp.zeros_like(sums)

        def clear(t, carry):
            km[:, pl.ds(pl.multiple_of(t * 256, 256), 256)] = jnp.zeros((2 * QB, 256), F32)
            return carry

        lax.fori_loop(tile0, jnp.maximum(base_of(qb) + WIN - 1, last) // 256 + 1, clear, 0)

        def mass(kb, carry):
            e = jnp.exp2(sbuf[kb - kb0] - peak)
            sums[...] = sums[...] + e[:, :128] + e[:, 128:]
            got = lax.dot_general(e.astype(BF16), marks[kb], NT, preferred_element_type=F32)
            lanes = pl.ds(pl.multiple_of(base_of(kb), 128), WIN)
            km[:, lanes] = km[:, lanes] + got
            return carry

        lax.fori_loop(kb0, qb + 1, mass, 0)
        scale = 1.0 / jnp.sum(sums[...], axis=1, keepdims=True)
        lead = jnp.maximum(span_smem[first] - core * OWN, 0) // 8 * 8
        row = jnp.concatenate([span_ref[pl.ds(qb * 2, 1), :], span_ref[pl.ds(qb * 2 + 1, 1), :]], axis=1)

        def gather_part(lo_row, n):
            ids = lax.broadcasted_iota(jnp.int32, (n, QB), 0) + (lead + lo_row + core * OWN)
            pick = jnp.where(ids == row, 1.0, 0.0).astype(BF16)
            at = pl.ds(pl.multiple_of(lead + lo_row, 8), n)

            def tile(t, carry):
                lanes = pl.ds(pl.multiple_of(t * 256, 256), 256)
                for h in range(2):
                    hs = slice(h * QB, (h + 1) * QB)
                    part = (km[hs, lanes] * scale[hs]).astype(BF16)
                    tot[h, at, lanes] = tot[h, at, lanes] + jnp.dot(pick, part, preferred_element_type=F32)
                return carry

            lax.fori_loop(tile0, last // 256 + 1, tile, 0)
            cnt[at, :] = cnt[at, :] + jnp.dot(pick, ones, preferred_element_type=F32)

        gather_part(*PARTS[0])

        @pl.when(last - core * OWN >= lead + PARTS[1][0])
        def _():
            gather_part(*PARTS[1])

        ready = (span_smem[jnp.minimum(first + QB, TOKENS - 1)] - core * OWN) // GROUP
        ready = jnp.where(qb + 1 == hi, OWN // GROUP, ready)
        lax.fori_loop(done, ready, finish, 0)
        return ready

    lax.fori_loop(lo, hi, block, 0)
    for n in range(OWN // GROUP):
        out_copy(n).wait()


def attention(q, k, ssq, table, documents, span_ids):
    vmem = pl.BlockSpec(memory_space=pltpu.VMEM)
    return pl.pallas_call(
        attention_kernel,
        name="attention",
        out_shape=jax.ShapeDtypeStruct((OWN, 2, NS), F32),
        in_specs=[pl.BlockSpec(memory_space=pl.ANY)] * 3 + [vmem] * 3 + [pl.BlockSpec(memory_space=pltpu.SMEM)],
        out_specs=pl.BlockSpec(memory_space=pl.ANY),
        scratch_shapes=[
            pltpu.VMEM(q.shape, BF16),
            pltpu.VMEM(k.shape, BF16),
            pltpu.VMEM(ssq.shape, F32),
            pltpu.VMEM((TOKENS, HD), BF16),
            pltpu.VMEM((TOKENS // KB, WIN, KB), BF16),
            pltpu.VMEM((2 * QB, HD), BF16),
            pltpu.VMEM((6, 2 * QB, KB), F32),
            pltpu.VMEM((2 * QB, 128), F32),
            pltpu.VMEM((2 * QB, 128), F32),
            pltpu.VMEM((2 * QB, NS + 256), F32),
            pltpu.VMEM((2, OWN + 272, NS), F32),
            pltpu.VMEM((OWN + 272, 128), F32),
            pltpu.VMEM((OWN, 2, NS), F32),
            pltpu.SemaphoreType.DMA((8,)),
            pltpu.SemaphoreType.DMA((3,)),
        ],
        compiler_params=pltpu.CompilerParams(vmem_limit_bytes=60 * 1024 * 1024),
    )(q, k, ssq, table, documents.reshape(16, 128), span_ids.reshape(16, 128), span_ids)


def angle_table():
    i = np.arange(HD // 2, dtype=np.float64)
    f = 500000.0 ** (-i / (HD // 2))
    w = 2.0 * np.pi / f
    s = (8192.0 / w - 1.0) / 3.0
    f = np.where(w < 2048.0, f, np.where(w > 8192.0, f / 8.0, (1.0 - s) * f / 8.0 + s * f))
    fine = np.arange(SUB, dtype=np.float64)[:, None] * f[None, :]
    coarse = np.arange(0, TOKENS, SUB, dtype=np.float64)[:, None] * f[None, :]
    rows = [
        np.concatenate([np.cos(fine), np.sin(fine)], axis=1),
        np.concatenate([np.cos(coarse), np.cos(coarse)], axis=1),
        np.concatenate([-np.sin(coarse), np.sin(coarse)], axis=1),
    ]
    return np.concatenate(rows, axis=0).astype(np.float32)


def local(tokens, norm_gain, query_weight, key_weight, documents, span_ids):
    q, k, ssq = project(tokens, norm_gain, query_weight, key_weight)
    table = jnp.asarray(angle_table())
    return attention(
        q.reshape(16, 2 * SUB, HD), k.reshape(TOKENS, HD), ssq, table, documents, span_ids
    )


def solution(mesh):
    finer = Mesh(
        mesh.devices.reshape(mesh.shape["blk"], 4, 4, mesh.shape["kv"]),
        (Y, X, Z, CORE),
    )
    return jax.shard_map(
        local,
        mesh=finer,
        in_specs=(P((Y, CORE), MP), P(MP), P(MP, Y), P(MP, Y), P(), P()),
        out_specs=P(CORE, BLK_MP, None),
        check_vma=False,
    )
```
